32 devices in a mesh: tile: 4 (over x, core), chan: 4 (over z), beam: 2 (over y).
Axes of the slice: x: 2, y: 2, z: 4, core: 2. Of those that a mesh axis runs over, the one named last changes fastest.
Arguments:
- voltages: bfloat16 [32, 128, 2, 2, 1536], P(None, 'tile', None, None, 'chan'), may hold values from -6 to 6
- calib_gain: float32 [128, 2, 2, 1536], P(('tile', 'beam'), None, None, 'chan'), may hold values from -0.375 to 0.375
- tile_flags: int32 [128], P(('tile', 'beam')), may hold values 0 or 1
- delays: float32 [64, 128], P(None, 'tile'), may hold values from -4 to 4
- pointing: int32 [2], P('beam'), may hold values from 0 to 63
- synth_filter: float32 [12, 128], replicated, may hold values from -0.5 to 0.5
Outputs:
- streams: float32 [32, 2, 2, 12, 256], P('tile', 'beam', None, 'chan')
The draws below stay inside these ranges and needn't reach their ends.
Inputs may be any that keep to these rules, and one draw needn't show every extreme that they name: `tile_flags`: 1 marks a tile in use. `pointing`: a row of delays, one of 64.
All inputs are finite; a program needn't handle non-finite values. No bound on the sum of `tile_flags` on one device may be relied on, other than what follows from the above.
Results may differ from the reference program's by a relative error of at most 0.0003.
Values sent between devices are 32-bit elements; how exact they have to be, the bound alone decides.
A program may use at most 64 MiB of HBM per device.

```python
import math
import jax
import jax.numpy as jnp
from jax import lax

NT = 128
K = 128
COARSE = 12
TAPS = 12
NPOINT = 64
T_SIZE = 32
BEAMS = 2
CHANS = 1536


def touch_ends(result, rng, low, top_value):
    spot = [jax.random.randint(jax.random.fold_in(rng, axis), (), 0, length) for axis, length in enumerate(result.shape)]
    widest = result.shape.index(max(result.shape))
    beside = spot[:widest] + [(spot[widest] + 1) % result.shape[widest]] + spot[widest + 1:]
    return result.at[tuple(spot)].set(low).at[tuple(beside)].set(top_value)


def spiked(entries, rng, source, target, blocks, factor):
    owner, partner = [(jnp.arange(entries.shape[axis_at]) // (entries.shape[axis_at] // blocks)).reshape([-1 if axis == axis_at else 1 for axis in range(entries.ndim)]) for axis_at in (source, target)]
    chosen = jax.random.permutation(rng, blocks)[partner]
    strong = (owner == chosen) | (owner == (partner + blocks // 2) % blocks)
    return jnp.where(strong, factor * entries, entries)


def block_scale(stream_key, extent, pieces, low, top_value):
    def one(dim, parts):
        steps = jax.random.uniform(jax.random.fold_in(jax.random.fold_in(stream_key, 6), dim), (parts,), jnp.float32, low / len(pieces), top_value / len(pieces))
        return jnp.repeat(jnp.exp(steps), extent[dim] // parts).reshape((-1,) + (1,) * (len(extent) - dim - 1))

    level = one(*pieces[0])
    for cut in pieces[1:]:
        level = level * one(*cut)
    return level


def noise(key, dims, deviation, limit, shards=(), kind=jnp.bfloat16):
    drawn = deviation * jax.random.normal(key, dims, jnp.float32)
    if shards:
        drawn = drawn * block_scale(key, dims, shards, -0.22, 0.18)
    return jnp.clip(drawn, -limit, limit).astype(kind)


def gaussian_with(own_key, dims, deviation, reach, split, heavy, kind=jnp.bfloat16):
    values = deviation * jax.random.normal(own_key, dims, jnp.float32)
    if split:
        values = values * block_scale(own_key, dims, split, -0.22, 0.18)
    return jnp.clip(spiked(values, jax.random.fold_in(own_key, 3), *heavy), -reach, reach).astype(kind)


def setup_inputs(seed: int = 0) -> dict:
    key_of = jax.random.split(jax.random.key(seed), 7)
    voltages = gaussian_with(key_of[0], (T_SIZE, NT, 2, 2, CHANS), 1.0, 6.0, ((1, 4), (4, 4)), (1, 0, 4, 2.0))
    calib_gain = noise(key_of[1], (NT, 2, 2, CHANS), (0.7 * NT ** -0.5), 0.375, ((0, 8), (3, 4)), jnp.float32)
    tile_flags = touch_ends((jax.random.randint(key_of[2], (NT,), 0, 4) < 3).astype(jnp.int32), jax.random.fold_in(key_of[2], 1), 0, 1)
    delays = jnp.clip(jax.random.uniform(key_of[3], (NPOINT, NT), jnp.float32, -4.0, 4.0) * block_scale(key_of[3], (NPOINT, NT), ((1, 4),), -0.4, 0.0), -4.0, 4.0)
    pointing = jax.random.randint(key_of[4], (BEAMS,), 0, NPOINT).astype(jnp.int32)
    synth_filter = jnp.clip(jax.random.uniform(key_of[5], (TAPS, K), jnp.float32, -0.5, 0.5), -0.5, 0.5)
    return {"voltages": voltages, "calib_gain": calib_gain, "tile_flags": tile_flags, "delays": delays, "pointing": pointing, "synth_filter": synth_filter}


TWO_PI = 6.283185307179586

def channel_frequency(first_index, length):
    global_idx = first_index + jnp.arange(length, dtype=jnp.int32)
    physical = global_idx % COARSE * K + global_idx // COARSE
    return (physical.astype(jnp.float32) + 0.5) / (K * COARSE)

def beam_weights(calib_gain, tile_flags, tile_delay, frequency):
    phase_angle = (TWO_PI * tile_delay)[:, :, None] * frequency[None, None, :]
    cosine = jnp.cos(phase_angle)[:, :, None, :]
    sine_part = jnp.sin(phase_angle)[:, :, None, :]
    gain_re = calib_gain[:, :, 0, :][None]
    gain_im = calib_gain[:, :, 1, :][None]
    in_use = tile_flags.astype(jnp.float32)[None, :, None, None]
    weight_re = in_use * (gain_re * cosine + gain_im * sine_part)
    weight_im = in_use * (gain_im * cosine - gain_re * sine_part)
    return (weight_re, weight_im)

def reference(voltages, calib_gain, tile_flags, delays, pointing, synth_filter):
    tile_delay = delays[pointing]
    frequency = channel_frequency(0, K * COARSE)
    weight_re, weight_im = beam_weights(calib_gain, tile_flags, tile_delay, frequency)
    row_count = voltages.shape[0]
    beams = pointing.shape[0]
    chans = voltages.shape[-1]

    def accumulate(carried, items):
        volt, tile_re, tile_im = items
        volt = volt.astype(jnp.float32)
        volt_re = volt[:, None, :, 0, :]
        volt_im = volt[:, None, :, 1, :]
        beam_re = carried[0] + (tile_re[None] * volt_re - tile_im[None] * volt_im)
        beam_im = carried[1] + (tile_re[None] * volt_im + tile_im[None] * volt_re)
        return ((beam_re, beam_im), None)
    zeros = jnp.zeros((row_count, beams, 2, chans), jnp.float32)
    (beam_re, beam_im), unused = lax.scan(accumulate, (zeros, zeros), (jnp.moveaxis(voltages, 1, 0), jnp.moveaxis(weight_re, 1, 0), jnp.moveaxis(weight_im, 1, 0)))
    grid_shape = (row_count, beams, 2, K, COARSE)
    combined = lax.complex(beam_re, beam_im).reshape(grid_shape)
    spectra = jnp.fft.ifft(combined, axis=3) * math.sqrt(K)
    spectra = jnp.moveaxis(spectra, 3, 4)
    padded = jnp.pad(spectra, ((TAPS - 1, 0), (0, 0), (0, 0), (0, 0), (0, 0)))
    streams = jnp.zeros_like(spectra)
    for offset in range(TAPS):
        begin = TAPS - 1 - offset
        streams = streams + synth_filter[offset] * padded[begin:begin + row_count]
    return jnp.concatenate([jnp.real(streams), jnp.imag(streams)], axis=-1)
```

```python
import functools
import math

import jax
import jax.numpy as jnp
import numpy as np
from jax import lax
from jax.experimental import pallas as pl
from jax.experimental.pallas import tpu as pltpu
from jax.sharding import PartitionSpec as P

COARSE = 12
LANES = 128
MESH = pl.DeviceIdType.MESH
F32 = jnp.float32
BF16 = jnp.bfloat16


def even_fit(func, degree):
    series = np.polynomial.chebyshev.Chebyshev.interpolate(
        lambda u: func(np.sqrt(u)), degree, domain=[0.0, 0.25]
    )
    return [float(v) for v in series.convert(kind=np.polynomial.Polynomial).coef]


COS_COEF = even_fit(lambda r: np.cos(2 * np.pi * r), 7)
SIN_COEF = even_fit(lambda r: 2 * np.pi * np.sinc(2 * r), 7)


def horner(coef, u):
    total = jnp.full_like(u, coef[-1])
    for value in coef[-2::-1]:
        total = total * u + value
    return total


def split_bf16(table):
    high = table.astype(BF16)
    low = (table - high.astype(np.float64)).astype(BF16)
    return high, low


def dft_table(nz, fz):
    k = nz * fz
    f = np.arange(k)
    m = np.arange(k)
    angle = 2 * np.pi * (f[:, None] * m[None, :] % k) / k
    cosine, sine = np.cos(angle) / math.sqrt(k), np.sin(angle) / math.sqrt(k)
    out = np.zeros((nz, 2, 2, fz, 2, 2, k))
    for p in range(2):
        out[:, p, 0, :, p, 0] = cosine.reshape(nz, fz, k)
        out[:, p, 0, :, p, 1] = sine.reshape(nz, fz, k)
        out[:, p, 1, :, p, 0] = -sine.reshape(nz, fz, k)
        out[:, p, 1, :, p, 1] = cosine.reshape(nz, fz, k)
    return split_bf16(out.reshape(nz * 4 * fz, 4 * k))


def gather_table(nz, fz, cz):
    width = fz * COARSE
    out = np.zeros((width, width), np.float64)
    for c in range(cz):
        for z in range(nz):
            for f in range(fz):
                out[f * COARSE + z * cz + c, (c * nz + z) * fz + f] = 1.0
    return out.astype(BF16)


def kernel(
    cfg,
    volt_ref,
    gain_ref,
    flag_src,
    delay_src,
    point_src,
    synth_src,
    table_src,
    out_ref,
    flag_ref,
    delay_ref,
    point_ref,
    synth_ref,
    table_ref,
    volt,
    own_gain,
    gains,
    w_re,
    w_im,
    acc,
    part,
    recv,
    packed,
    inbox,
    spec,
    small_sem,
    own_sem,
    volt_sem,
    gain_send,
    gain_recv,
    part_send,
    part_recv,
    pack_send,
    pack_recv,
):
    nt, nz, nb, tb, n_all, taps, fz, cz, halo, exchange = cfg
    tile = lax.axis_index("tile")
    chan = lax.axis_index("chan")
    beam = lax.axis_index("beam")
    rows_t = n_all * 4

    def peer(t, z, b):
        return {"tile": t, "chan": z, "beam": b}

    pair = 2 if nt % 2 == 0 else 1
    chips = nt // pair
    chip, core = lax.div(tile, pair), lax.rem(tile, pair)
    order = [
        (a, k)
        for a in sorted(range(1, chips), key=lambda a: abs(2 * a - chips))
        for k in range(pair)
    ] + [(0, k) for k in range(pair - 1, -1, -1)]

    def time_block(slot):
        a, k = order[slot]
        return lax.rem(chip + a, chips) * pair + lax.rem(core + k, pair)

    def wait_all(ref, sem):
        pltpu.make_async_copy(ref, ref, sem).wait()

    gain_rows = gain_ref.reshape(gain_ref.shape[0] * 2, gain_ref.shape[2])
    for c in range(cz):
        pltpu.make_async_copy(
            gain_rows.at[:, pl.ds(c * LANES, LANES)], own_gain.at[c], own_sem.at[0]
        ).start()
    small = [
        pltpu.make_async_copy(src, dst, small_sem.at[i])
        for i, (src, dst) in enumerate(
            [
                (flag_src, flag_ref),
                (point_src, point_ref),
                (delay_src, delay_ref),
                (synth_src, synth_ref),
                (table_src, table_ref),
            ]
        )
    ]
    for copy in small[:3]:
        copy.start()

    barrier = pltpu.get_barrier_semaphore()
    count = 0
    for dt in range(nt):
        for dz in range(nz):
            if dt or dz:
                pl.semaphore_signal(
                    barrier,
                    inc=1,
                    device_id=peer(lax.rem(tile + dt, nt), lax.rem(chan + dz, nz), beam),
                    device_id_type=MESH,
                )
                count += 1
    for db in range(1, nb):
        pl.semaphore_signal(
            barrier, inc=1, device_id=peer(tile, chan, lax.rem(beam + db, nb)), device_id_type=MESH
        )
        count += 1

    volt_rows = volt_ref.reshape(volt_ref.shape[0] * 2, volt_ref.shape[2])
    for c in range(cz):
        for slot in range(nt):
            pltpu.make_async_copy(
                volt_rows.at[
                    pl.ds(time_block(slot) * (tb * rows_t), tb * rows_t), pl.ds(c * LANES, LANES)
                ],
                volt.at[slot, c],
                volt_sem.at[c],
            ).start()
    for copy in small[3:]:
        copy.start()

    row = lax.broadcasted_iota(jnp.int32, (8, LANES), 0)
    first = row < 4
    n_own = n_all // nb
    share = n_own * 4 if exchange else rows_t
    even = lax.rem(lax.broadcasted_iota(jnp.int32, (share, LANES), 0), 2) == 0

    with jax.named_scope("ownload"):
        wait_all(own_gain, own_sem.at[0])
        small[0].wait()
    if exchange:
        use = jnp.concatenate(
            [
                jnp.where(first, flag_ref[2 * i].astype(F32), flag_ref[2 * i + 1].astype(F32))
                for i in range(n_own // 2)
            ],
            axis=0,
        )
        for c in range(cz):
            gains[beam, c] = use * own_gain[c]

    for h in range(1, halo + 1):

        @pl.when(tile < h)
        def _():
            inbox[h] = jnp.zeros(inbox.shape[1:], F32)

    unused = halo * tb - (taps - 1)
    if unused:
        inbox[halo, :, :, pl.ds(0, unused), :] = jnp.zeros((nz, cz, unused, LANES), F32)

    with jax.named_scope("barrier"):
        pl.semaphore_wait(barrier, count)

    if exchange:
        for c in range(cz):
            for db in range(1, nb):
                pltpu.make_async_remote_copy(
                    src_ref=gains.at[beam, c],
                    dst_ref=gains.at[beam, c],
                    send_sem=gain_send.at[0],
                    recv_sem=gain_recv.at[c],
                    device_id=peer(tile, chan, lax.rem(beam + db, nb)),
                    device_id_type=MESH,
                ).start()

    for copy in small[1:3]:
        copy.wait()
    select = lax.broadcasted_iota(jnp.int32, delay_ref.shape, 1) == point_ref[0]
    delay = jnp.sum(jnp.where(select, delay_ref[...], 0.0), axis=1, keepdims=True)
    delay = jnp.broadcast_to(delay, (n_all, LANES))
    delay = jnp.concatenate(
        [
            jnp.where(
                first,
                jnp.broadcast_to(delay[2 * i : 2 * i + 1], (8, LANES)),
                jnp.broadcast_to(delay[2 * i + 1 : 2 * i + 2], (8, LANES)),
            )
            for i in range(n_all // 2)
        ],
        axis=0,
    )
    for c in range(cz):
        local = (lax.broadcasted_iota(jnp.int32, (1, LANES), 1) + c * LANES).astype(F32)
        fine = jnp.floor((local + 0.5) / COARSE)
        channel = (local - COARSE * fine) * (nz * fz) + fine + (chan * fz).astype(F32)
        frequency = (channel + 0.5) / (COARSE * nz * fz)
        cycles = delay * frequency
        turn = cycles - jnp.floor(cycles + 0.5)
        square = turn * turn
        w_re[c] = horner(COS_COEF, square)
        w_im[c] = turn * horner(SIN_COEF, square)

    def weigh(c, start, gain):
        rows = pl.ds(start, share)
        swapped = jnp.where(even, pltpu.roll(gain, share - 1, 0), -pltpu.roll(gain, 1, 0))
        weight = gain * w_re[c, rows, :] + swapped * w_im[c, rows, :]
        w_re[c, rows, :] = jnp.where(even, weight, pltpu.roll(weight, 1, 0))
        w_im[c, rows, :] = jnp.where(even, pltpu.roll(weight, share - 1, 0), weight)

    unroll = math.gcd(tb, 8)

    def accumulate(slot, c, starts, extend):
        def step(s, carry):
            sums = [[jnp.zeros((16, LANES), F32)] * 2 for _ in range(unroll)]
            for start in starts:
                for q in range(share // 16):
                    at = start + q * 16
                    wr = w_re[c, pl.ds(at, 16), :]
                    wi = w_im[c, pl.ds(at, 16), :]
                    for u in range(unroll):
                        begin = pl.multiple_of((s * unroll + u) * rows_t + at, 16)
                        v = volt[slot, c, pl.ds(begin, 16), :].astype(F32)
                        sums[u] = [sums[u][0] + wr * v, sums[u][1] + wi * v]
            for u in range(unroll):
                begin = pl.multiple_of((s * unroll + u) * 16, 16)
                for which in range(2):
                    value = sums[u][which]
                    value = value[:8] + value[8:]
                    rows = pl.ds(begin + which * 8, 8)
                    acc[slot, c, rows, :] = acc[slot, c, rows, :] + value if extend else value
            return carry

        if tb == unroll:
            step(0, 0)
        else:
            lax.fori_loop(0, tb // unroll, step, 0)

    def take(slot, c, which, p, ri):
        total = None
        for half in range(2):
            value = acc[slot, c, pl.ds(which * 8 + half * 4 + p * 2 + ri, tb, stride=16), :]
            total = value if total is None else total + value
        return total

    starts = [0]
    if exchange:
        starts = [pl.multiple_of(lax.rem(beam + db, nb) * share, 16) for db in range(nb)]
    with jax.named_scope("acc1"):
        for c in range(cz):
            weigh(c, starts[0], gains[beam, c] if exchange else own_gain[c])
            if exchange:
                wait_all(volt.at[:, c], volt_sem.at[c])

                def first_sum(slot, carry, c=c):
                    accumulate(slot, c, starts[:1], False)
                    return carry

                lax.fori_loop(0, nt, first_sum, 0)
    for c in range(cz):
        with jax.named_scope(f"gainwait{c}"):
            if exchange:
                wait_all(gains.at[pl.ds(0, nb - 1), c], gain_recv.at[c])
            else:
                wait_all(volt.at[:, c], volt_sem.at[c])
        for db in range(1, nb if exchange else 1):
            weigh(c, starts[db], gains[lax.rem(beam + db, nb), c])
        for slot in range(nt):
            if exchange:
                accumulate(slot, c, starts[1:], True)
            else:
                accumulate(slot, c, starts, False)
            for p in range(2):
                part[slot, c, p * 2] = take(slot, c, 0, p, 0) - take(slot, c, 1, p, 1)
                part[slot, c, p * 2 + 1] = take(slot, c, 0, p, 1) + take(slot, c, 1, p, 0)
            if slot < nt - 1:
                pltpu.make_async_remote_copy(
                    src_ref=part.at[slot, c],
                    dst_ref=recv.at[slot, c],
                    send_sem=part_send.at[0],
                    recv_sem=part_recv.at[c],
                    device_id=peer(time_block(slot), chan, beam),
                    device_id_type=MESH,
                ).start()

    for copy in small[3:]:
        copy.wait()
    kdim = 4 * nz * fz
    moved = jnp.zeros((4 * tb, cz * LANES), F32)
    for c in range(cz):
        with jax.named_scope(f"partwait{c}"):
            wait_all(recv.at[:, c], part_recv.at[c])
        sums = part[nt - 1, c]
        for slot in range(nt - 1):
            sums = sums + recv[slot, c]
        sums = sums.reshape(4 * tb, LANES)
        high = sums.astype(BF16)
        low = (sums - high.astype(F32)).astype(BF16)
        table = table_ref[pl.ds(2 * kdim + c * LANES, LANES), pl.ds(0, cz * LANES)]
        moved = moved + jnp.dot(high, table, preferred_element_type=F32)
        moved = moved + jnp.dot(low, table, preferred_element_type=F32)
    group = lax.broadcasted_iota(jnp.int32, (tb, LANES), 1) // fz
    for z in range(nz):
        for c in range(cz):
            total = None
            for g in range(4):
                value = moved[g * tb : (g + 1) * tb, c * LANES : (c + 1) * LANES]
                shift = (g - z) * fz % LANES
                if shift:
                    value = pltpu.roll(value, shift, 1)
                total = value if g == 0 else jnp.where(group == g, value, total)
            packed[z, c] = total

    half = 2 * chan // nz
    place = chan * half + (nz - 1 - chan) * (1 - half)

    def target(i):
        if i == nz - 1:
            return chan
        other = i + (i + nz - place) // nz
        return other * half + (nz - 1 - other) * (1 - half)

    def halo_rows(h):
        count = tb if h < halo else taps - 1 - (halo - 1) * tb
        return pl.ds(tb - count, count)

    messages = [(h, i) for i in range(nz) for h in range(halo + 1) if h or i < nz - 1]

    for h, i in messages:

        def send(h=h, i=i):
            pltpu.make_async_remote_copy(
                src_ref=packed.at[target(i), :, halo_rows(h), :],
                dst_ref=inbox.at[h, chan, :, halo_rows(h), :],
                send_sem=pack_send.at[h],
                recv_sem=pack_recv.at[h],
                device_id=peer(lax.rem(tile + h, nt), target(i), beam),
                device_id_type=MESH,
            ).start()

        if h == 0:
            send()
        else:
            pl.when(tile + h < nt)(send)

    inbox[0, chan] = packed[chan]

    with jax.named_scope("packwait"):
        for h in range(halo + 1):
            if h == 0:
                wait_all(inbox.at[0, pl.ds(0, nz - 1)], pack_recv.at[0])
            else:

                @pl.when(tile >= h)
                def _():
                    wait_all(inbox.at[h, :, :, halo_rows(h), :], pack_recv.at[h])

    lhs = jnp.concatenate(
        [
            jnp.concatenate([inbox[h, z, c] for z in range(nz)], axis=1)
            for c in range(cz)
            for h in range(halo, -1, -1)
        ],
        axis=0,
    )
    high = lhs.astype(BF16)
    low = (lhs - high.astype(F32)).astype(BF16)
    spec[...] = (
        jnp.dot(high, table_ref[pl.ds(0, kdim), :], preferred_element_type=F32)
        + jnp.dot(low, table_ref[pl.ds(0, kdim), :], preferred_element_type=F32)
        + jnp.dot(high, table_ref[pl.ds(kdim, kdim), :], preferred_element_type=F32)
    )
    span = (halo + 1) * tb
    for c in range(cz):
        for g in range(4):
            total = None
            for k in range(taps):
                value = synth_ref[pl.ds(k, 1), :] * spec[
                    pl.ds(c * span + halo * tb - k, tb), g * LANES : (g + 1) * LANES
                ]
                total = value if total is None else total + value
            for t in range(tb):
                out_ref[t, c, pl.ds(g // 2, 1), (g % 2) * LANES : (g % 2 + 1) * LANES] = total[t : t + 1]

    with jax.named_scope("sendwait"):
        if exchange:
            wait_all(gains.at[pl.ds(0, nb - 1)], gain_send.at[0])
        wait_all(recv, part_send.at[0])
        for h in range(halo + 1):
            if h == 0:
                wait_all(packed.at[pl.ds(0, nz - 1)], pack_send.at[0])
            else:

                @pl.when(tile + h < nt)
                def _():
                    wait_all(packed.at[:, :, halo_rows(h), :], pack_send.at[h])


def store(value_ref, out_ref, sem):
    copy = pltpu.make_async_copy(value_ref, out_ref, sem)
    copy.start()
    copy.wait()


def body(mesh, voltages, calib_gain, tile_flags, delays, pointing, synth_filter):
    nt, nz, nb = mesh.shape["tile"], mesh.shape["chan"], mesh.shape["beam"]
    total_rows, n_all = voltages.shape[:2]
    width = voltages.shape[-1]
    taps, k = synth_filter.shape
    tb = total_rows // nt
    fz = width // COARSE
    cz = COARSE // nz
    halo = -(-(taps - 1) // tb)
    n_own = calib_gain.shape[0]
    exchange = n_own % 4 == 0 and mesh.shape["beam"] > 1
    gain = calib_gain
    if not exchange:
        gain = gain * tile_flags.astype(F32)[:, None, None, None]
        gain = lax.all_gather(gain, "beam", axis=0, tiled=True)
    perm = gather_table(nz, fz, cz)
    perm = np.pad(perm, ((0, 0), (0, 4 * k - perm.shape[1])))
    table = np.concatenate([*dft_table(nz, fz), perm])
    cfg = (nt, nz, nb, tb, n_all, taps, fz, cz, halo, exchange)
    vmem = pl.BlockSpec(memory_space=pltpu.VMEM)
    anywhere = pl.BlockSpec(memory_space=pltpu.HBM)
    span = (halo + 1) * tb
    dma = pltpu.SemaphoreType.DMA
    out = pl.pallas_call(
        functools.partial(kernel, cfg),
        out_shape=pltpu.VMEM((tb, cz, 2, 2 * k), F32),
        in_specs=[anywhere] * 7,
        out_specs=vmem,
        scratch_shapes=[
            pltpu.SMEM(tile_flags.shape, jnp.int32),
            pltpu.VMEM(delays.shape[::-1], F32),
            pltpu.SMEM(pointing.shape, jnp.int32),
            pltpu.VMEM(synth_filter.shape, F32),
            pltpu.VMEM(table.shape, BF16),
            pltpu.VMEM((nt, cz, tb * n_all * 4, LANES), BF16),
            pltpu.VMEM((cz, gain.shape[0] * 4, LANES), F32),
            pltpu.VMEM((nb, cz, n_own * 4, LANES), F32),
            pltpu.VMEM((cz, n_all * 4, LANES), F32),
            pltpu.VMEM((cz, n_all * 4, LANES), F32),
            pltpu.VMEM((nt, cz, tb * 16, LANES), F32),
            pltpu.VMEM((nt, cz, 4, tb, LANES), F32),
            pltpu.VMEM((nt - 1, cz, 4, tb, LANES), F32),
            pltpu.VMEM((nz, cz, tb, LANES), F32),
            pltpu.VMEM((halo + 1, nz, cz, tb, LANES), F32),
            pltpu.VMEM((cz * span, 4 * k), F32),
            dma((5,)),
            dma((1,)),
            dma((cz,)),
            dma((1,)),
            dma((cz,)),
            dma((1,)),
            dma((cz,)),
            dma((halo + 1,)),
            dma((halo + 1,)),
        ],
        compiler_params=pltpu.CompilerParams(collective_id=0, has_side_effects=True),
    )(
        voltages.reshape(-1, 2, width),
        gain.reshape(-1, 2, width),
        tile_flags,
        delays.T,
        pointing,
        synth_filter,
        jnp.asarray(table),
    )
    final = pl.pallas_call(
        store,
        out_shape=jax.ShapeDtypeStruct(out.shape, F32),
        in_specs=[vmem],
        out_specs=pl.BlockSpec(memory_space=pltpu.HBM),
        scratch_shapes=[dma(())],
    )(pltpu.with_memory_space_constraint(out, pltpu.VMEM))
    return final.transpose(0, 2, 1, 3)[:, None]


def solution(mesh):
    in_specs = (
        P(None, "tile", None, None, "chan"),
        P(("tile", "beam"), None, None, "chan"),
        P(("tile", "beam")),
        P(None, "tile"),
        P("beam"),
        P(),
    )
    out_specs = P("tile", "beam", None, "chan", None)
    return jax.shard_map(
        functools.partial(body, mesh), mesh=mesh, in_specs=in_specs, out_specs=out_specs, check_vma=False
    )
```

```python
import functools
import math

import jax
import jax.numpy as jnp
import numpy as np
from jax import lax
from jax.experimental import pallas as pl
from jax.experimental.pallas import tpu as pltpu
from jax.sharding import PartitionSpec as P

COARSE = 12
LANES = 128
MESH = pl.DeviceIdType.MESH
F32 = jnp.float32
BF16 = jnp.bfloat16


def even_fit(func, degree):
    series = np.polynomial.chebyshev.Chebyshev.interpolate(
        lambda u: func(np.sqrt(u)), degree, domain=[0.0, 0.25]
    )
    return [float(v) for v in series.convert(kind=np.polynomial.Polynomial).coef]


COS_COEF = even_fit(lambda r: np.cos(2 * np.pi * r), 7)
SIN_COEF = even_fit(lambda r: 2 * np.pi * np.sinc(2 * r), 7)


def horner(coef, u):
    total = jnp.full_like(u, coef[-1])
    for value in coef[-2::-1]:
        total = total * u + value
    return total


def split_bf16(table):
    high = table.astype(BF16)
    low = (table - high.astype(np.float64)).astype(BF16)
    return high, low


def dft_table(nz, fz):
    k = nz * fz
    f = np.arange(k)
    m = np.arange(k)
    angle = 2 * np.pi * (f[:, None] * m[None, :] % k) / k
    cosine, sine = np.cos(angle) / math.sqrt(k), np.sin(angle) / math.sqrt(k)
    out = np.zeros((nz, 2, 2, fz, 2, 2, k))
    for p in range(2):
        out[:, p, 0, :, p, 0] = cosine.reshape(nz, fz, k)
        out[:, p, 0, :, p, 1] = sine.reshape(nz, fz, k)
        out[:, p, 1, :, p, 0] = -sine.reshape(nz, fz, k)
        out[:, p, 1, :, p, 1] = cosine.reshape(nz, fz, k)
    return split_bf16(out.reshape(nz * 4 * fz, 4 * k))


def gather_table(nz, fz, cz):
    width = fz * COARSE
    out = np.zeros((width, width), np.float64)
    for c in range(cz):
        for z in range(nz):
            for f in range(fz):
                out[f * COARSE + z * cz + c, (c * nz + z) * fz + f] = 1.0
    return out.astype(BF16)


def kernel(
    cfg,
    volt_ref,
    gain_ref,
    flag_src,
    delay_src,
    point_src,
    synth_src,
    perm_src,
    dft_src,
    out_ref,
    flag_ref,
    delay_ref,
    point_ref,
    synth_ref,
    perm_ref,
    dft_ref,
    volt,
    own_gain,
    gains,
    w_re,
    w_im,
    acc,
    part,
    recv,
    packed,
    inbox,
    spec,
    small_sem,
    own_sem,
    volt_sem,
    gain_send,
    gain_recv,
    part_send,
    part_recv,
    pack_send,
    pack_recv,
    dft_sem,
):
    nt, nz, nb, tb, n_all, taps, fz, cz, halo, exchange = cfg
    tile = lax.axis_index("tile")
    chan = lax.axis_index("chan")
    beam = lax.axis_index("beam")
    rows_t = n_all * 4

    def peer(t, z, b):
        return {"tile": t, "chan": z, "beam": b}

    pair = 2 if nt % 2 == 0 else 1
    chips = nt // pair
    chip, core = lax.div(tile, pair), lax.rem(tile, pair)
    packer = pair - 1
    packs = core == packer
    order = sorted(range(1, chips), key=lambda a: abs(2 * a - chips)) + [0]
    block = pair * tb

    def chip_of(slot):
        return lax.rem(chip + order[slot], chips)

    def packer_of(target_chip):
        return target_chip * pair + packer

    def wait_all(ref, sem):
        pltpu.make_async_copy(ref, ref, sem).wait()

    gain_rows = gain_ref.reshape(gain_ref.shape[0] * 2, gain_ref.shape[2])
    for c in range(cz):
        pltpu.make_async_copy(
            gain_rows.at[:, pl.ds(c * LANES, LANES)], own_gain.at[c], own_sem.at[0]
        ).start()
    small = [
        pltpu.make_async_copy(src, dst, small_sem.at[i])
        for i, (src, dst) in enumerate(
            [
                (flag_src, flag_ref),
                (point_src, point_ref),
                (delay_src, delay_ref),
                (synth_src, synth_ref),
                (perm_src, perm_ref),
            ]
        )
    ]
    dft_copies = [
        pltpu.make_async_copy(
            dft_src.at[:, g], dft_ref.at[:, lax.rem(chan + g, 4)], dft_sem.at[0]
        )
        for g in range(4)
    ]
    for copy in small[:3]:
        copy.start()

    barrier = pltpu.get_barrier_semaphore()

    def greet(t, z, b):
        pl.semaphore_signal(barrier, inc=1, device_id=peer(t, z, b), device_id_type=MESH)

    for db in range(1, nb):
        greet(tile, chan, lax.rem(beam + db, nb))
    if pair > 1:

        @pl.when(packs)
        def _():
            for a in range(chips):
                for k in range(packer):
                    greet(lax.rem(chip + a, chips) * pair + k, chan, beam)

        @pl.when(jnp.logical_not(packs))
        def _():
            for a in range(chips):
                greet(packer_of(lax.rem(chip + a, chips)), chan, beam)

    for dz in range(nz):
        for a in range(chips):
            if dz == 0:
                if a:
                    pl.when(packs)(
                        functools.partial(greet, packer_of(lax.rem(chip + a, chips)), chan, beam)
                    )
            else:
                greet(packer_of(lax.rem(chip + a, chips)), lax.rem(chan + dz, nz), beam)

    few = chips * (pair - 1) // max(packer, 1) + nb - 1
    many = nt * nz - 1 + nb - 1

    volt_rows = volt_ref.reshape(volt_ref.shape[0] * 2, volt_ref.shape[2])
    for c in range(cz):
        for slot in range(chips):
            pltpu.make_async_copy(
                volt_rows.at[
                    pl.ds(chip_of(slot) * (block * rows_t), block * rows_t), pl.ds(c * LANES, LANES)
                ],
                volt.at[slot, c],
                volt_sem.at[c],
            ).start()
    for copy in small[3:] + dft_copies:
        copy.start()

    row = lax.broadcasted_iota(jnp.int32, (8, LANES), 0)
    first = row < 4
    n_own = n_all // nb
    share = n_own * 4 if exchange else rows_t
    even = lax.rem(lax.broadcasted_iota(jnp.int32, (share, LANES), 0), 2) == 0

    with jax.named_scope("ownload"):
        wait_all(own_gain, own_sem.at[0])
        small[0].wait()
    if exchange:
        use = jnp.concatenate(
            [
                jnp.where(first, flag_ref[2 * i].astype(F32), flag_ref[2 * i + 1].astype(F32))
                for i in range(n_own // 2)
            ],
            axis=0,
        )
        for c in range(cz):
            gains[beam, c] = use * own_gain[c]

    reach = -(-(taps - 1) // block)

    def rows_of(back, k):
        shift = (halo - k) * tb - back * block
        low = max(0, halo * tb - (taps - 1) - shift)
        high = min(block, (halo + 1) * tb - shift)
        return low, max(high - low, 0), low + shift

    unused = halo * tb - (taps - 1)
    if unused:
        inbox[:, :, pl.ds(0, unused), :] = jnp.zeros((nz, cz, unused, LANES), F32)
    for back in range(1, reach + 1):
        for k in range(pair):
            size, start = rows_of(back, k)[1:]
            if size:

                @pl.when(jnp.logical_and(chip < back, core == k))
                def _(size=size, start=start):
                    inbox[:, :, pl.ds(start, size), :] = jnp.zeros((nz, cz, size, LANES), F32)

    with jax.named_scope("barrier"):
        pl.semaphore_wait(barrier, few + core // max(packer, 1) * (many - few) if pair > 1 else many)

    if exchange:
        for c in range(cz):
            for db in range(1, nb):
                pltpu.make_async_remote_copy(
                    src_ref=gains.at[beam, c],
                    dst_ref=gains.at[beam, c],
                    send_sem=gain_send.at[0],
                    recv_sem=gain_recv.at[c],
                    device_id=peer(tile, chan, lax.rem(beam + db, nb)),
                    device_id_type=MESH,
                ).start()

    for copy in small[1:3]:
        copy.wait()
    select = lax.broadcasted_iota(jnp.int32, delay_ref.shape, 1) == point_ref[0]
    delay = jnp.sum(jnp.where(select, delay_ref[...], 0.0), axis=1, keepdims=True)
    delay = jnp.broadcast_to(delay, (n_all, LANES))
    delay = jnp.concatenate(
        [
            jnp.where(
                first,
                jnp.broadcast_to(delay[2 * i : 2 * i + 1], (8, LANES)),
                jnp.broadcast_to(delay[2 * i + 1 : 2 * i + 2], (8, LANES)),
            )
            for i in range(n_all // 2)
        ],
        axis=0,
    )
    for c in range(cz):
        local = (lax.broadcasted_iota(jnp.int32, (1, LANES), 1) + c * LANES).astype(F32)
        fine = jnp.floor((local + 0.5) / COARSE)
        channel = (local - COARSE * fine) * (nz * fz) + fine + (chan * fz).astype(F32)
        frequency = (channel + 0.5) / (COARSE * nz * fz)
        cycles = delay * frequency
        turn = cycles - jnp.floor(cycles + 0.5)
        square = turn * turn
        w_re[c] = horner(COS_COEF, square)
        w_im[c] = turn * horner(SIN_COEF, square)

    def weigh(c, start, gain):
        rows = pl.ds(start, share)
        swapped = jnp.where(even, pltpu.roll(gain, share - 1, 0), -pltpu.roll(gain, 1, 0))
        weight = gain * w_re[c, rows, :] + swapped * w_im[c, rows, :]
        w_re[c, rows, :] = jnp.where(even, weight, pltpu.roll(weight, 1, 0))
        w_im[c, rows, :] = jnp.where(even, pltpu.roll(weight, share - 1, 0), weight)

    unroll = math.gcd(block, 8)

    def accumulate(slot, c, starts, extend):
        def step(s, carry):
            sums = [[jnp.zeros((16, LANES), F32)] * 2 for _ in range(unroll)]
            for start in starts:
                for q in range(share // 16):
                    at = start + q * 16
                    wr = w_re[c, pl.ds(at, 16), :]
                    wi = w_im[c, pl.ds(at, 16), :]
                    for u in range(unroll):
                        begin = pl.multiple_of((s * unroll + u) * rows_t + at, 16)
                        v = volt[slot, c, pl.ds(begin, 16), :].astype(F32)
                        sums[u] = [sums[u][0] + wr * v, sums[u][1] + wi * v]
            for u in range(unroll):
                begin = pl.multiple_of((s * unroll + u) * 16, 16)
                for which in range(2):
                    value = sums[u][which]
                    value = value[:8] + value[8:]
                    rows = pl.ds(begin + which * 8, 8)
                    acc[slot, c, rows, :] = acc[slot, c, rows, :] + value if extend else value
            return carry

        lax.fori_loop(0, block // unroll, step, 0)

    def take(slot, c, which, p, ri):
        total = None
        for half in range(2):
            value = acc[slot, c, pl.ds(which * 8 + half * 4 + p * 2 + ri, block, stride=16), :]
            total = value if total is None else total + value
        return total

    starts = [0]
    if exchange:
        starts = [pl.multiple_of(lax.rem(beam + db, nb) * share, 16) for db in range(nb)]
    with jax.named_scope("acc1"):
        for c in range(cz):
            weigh(c, starts[0], gains[beam, c] if exchange else own_gain[c])
            if exchange:
                wait_all(volt.at[:, c], volt_sem.at[c])

                def first_sum(slot, carry, c=c):
                    accumulate(slot, c, starts[:1], False)
                    return carry

                lax.fori_loop(0, chips, first_sum, 0)
    for c in range(cz):
        with jax.named_scope(f"gainwait{c}"):
            if exchange:
                wait_all(gains.at[pl.ds(0, nb - 1), c], gain_recv.at[c])
            else:
                wait_all(volt.at[:, c], volt_sem.at[c])
        for db in range(1, nb if exchange else 1):
            weigh(c, starts[db], gains[lax.rem(beam + db, nb), c])
        for slot in range(chips):
            if exchange:
                accumulate(slot, c, starts[1:], True)
            else:
                accumulate(slot, c, starts, False)
            for p in range(2):
                part[slot, c, p * 2] = take(slot, c, 0, p, 0) - take(slot, c, 1, p, 1)
                part[slot, c, p * 2 + 1] = take(slot, c, 0, p, 1) + take(slot, c, 1, p, 0)
            def send(slot=slot, c=c):
                pltpu.make_async_remote_copy(
                    src_ref=part.at[slot, c],
                    dst_ref=recv.at[slot * pair + core, c],
                    send_sem=part_send.at[slot],
                    recv_sem=part_recv.at[c],
                    device_id=peer(packer_of(chip_of(slot)), chan, beam),
                    device_id_type=MESH,
                ).start()

            if slot < chips - 1:
                send()
            elif pair > 1:
                pl.when(jnp.logical_not(packs))(send)

    half = 2 * chan // nz
    place = chan * half + (nz - 1 - chan) * (1 - half)

    def target(i):
        if i == nz - 1:
            return chan
        other = i + (i + nz - place) // nz
        return other * half + (nz - 1 - other) * (1 - half)

    for copy in small[3:]:
        copy.wait()

    @pl.when(packs)
    def _():
        moved = jnp.zeros((4 * block, cz * LANES), F32)
        for c in range(cz):
            with jax.named_scope(f"partwait{c}"):
                wait_all(recv.at[:, c], part_recv.at[c])
            sums = part[chips - 1, c]
            for i in range(nt - 1):
                sums = sums + recv[i, c]
            sums = sums.reshape(4 * block, LANES)
            high = sums.astype(BF16)
            low = (sums - high.astype(F32)).astype(BF16)
            table = perm_ref[pl.ds(c * LANES, LANES), :]
            both = jnp.dot(
                jnp.concatenate([high, low], axis=0), table, preferred_element_type=F32
            )
            moved = moved + both[: 4 * block] + both[4 * block :]
        group = lax.broadcasted_iota(jnp.int32, (block, LANES), 1) // fz
        for c in range(cz):
            turned = []
            for g in range(4):
                value = moved[g * block : (g + 1) * block, c * LANES : (c + 1) * LANES]
                turned.append(pltpu.roll(value, g * fz, 1) if g else value)
            for z in range(nz):
                total = turned[0]
                for g in range(1, 4):
                    total = jnp.where(group == (g + z) % 4, turned[g], total)
                packed[z, c] = total

        for i in range(nz):
            for back in range(reach + 1):
                for k in range(pair):
                    begin, size, start = rows_of(back, k)
                    if not size or (i == nz - 1 and back == 0 and k == packer):
                        continue

                    def send(i=i, back=back, k=k, begin=begin, size=size, start=start):
                        pltpu.make_async_remote_copy(
                            src_ref=packed.at[target(i), :, pl.ds(begin, size), :],
                            dst_ref=inbox.at[chan, :, pl.ds(start, size), :],
                            send_sem=pack_send.at[back, k],
                            recv_sem=pack_recv.at[back],
                            device_id=peer(lax.rem(chip + back, chips) * pair + k, target(i), beam),
                            device_id_type=MESH,
                        ).start()

                    if back == 0:
                        send()
                    else:
                        pl.when(chip + back < chips)(send)

        begin, size, start = rows_of(0, packer)
        inbox[chan, :, pl.ds(start, size), :] = packed[chan, :, pl.ds(begin, size), :]

    for copy in dft_copies:
        copy.wait()

    def each_group(sends):
        for back in range(reach + 1):
            for k in range(pair):
                begin, size, start = rows_of(back, k)
                if not size:
                    continue
                count = nz - 1 if back == 0 and k == packer else nz
                there = packs if sends else core == k
                if back:
                    there = jnp.logical_and(there, chip + back < chips if sends else chip >= back)

                @pl.when(there)
                def _(back=back, k=k, count=count, begin=begin, size=size, start=start):
                    if sends:
                        wait_all(packed.at[pl.ds(0, count), :, pl.ds(begin, size), :], pack_send.at[back, k])
                    else:
                        wait_all(inbox.at[pl.ds(0, count), :, pl.ds(start, size), :], pack_recv.at[back])

    with jax.named_scope("packwait"):
        each_group(False)

    lhs = jnp.concatenate(
        [jnp.concatenate([inbox[z, c] for z in range(nz)], axis=1) for c in range(cz)], axis=0
    )
    high = lhs.astype(BF16)
    low = (lhs - high.astype(F32)).astype(BF16)
    kdim = nz * 4 * fz
    dft_h = dft_ref[:nz].reshape(kdim, 4 * nz * fz)
    dft_l = dft_ref[nz:].reshape(kdim, 4 * nz * fz)
    both = jnp.dot(jnp.concatenate([high, low], axis=0), dft_h, preferred_element_type=F32)
    half_rows = lhs.shape[0]
    spec[...] = (
        both[:half_rows] + both[half_rows:] + jnp.dot(high, dft_l, preferred_element_type=F32)
    )
    span = (halo + 1) * tb
    for c in range(cz):
        for g in range(4):
            total = None
            for k in range(taps):
                value = synth_ref[pl.ds(k, 1), :] * spec[
                    pl.ds(c * span + halo * tb - k, tb), g * LANES : (g + 1) * LANES
                ]
                total = value if total is None else total + value
            for t in range(tb):
                out_ref[t, c, pl.ds(g // 2, 1), (g % 2) * LANES : (g % 2 + 1) * LANES] = total[t : t + 1]

    with jax.named_scope("sendwait"):
        if exchange:
            wait_all(gains.at[pl.ds(0, nb - 1)], gain_send.at[0])
        for slot in range(chips):
            if slot < chips - 1:
                wait_all(part.at[slot], part_send.at[slot])
            elif pair > 1:

                @pl.when(jnp.logical_not(packs))
                def _():
                    wait_all(part.at[chips - 1], part_send.at[chips - 1])

        each_group(True)


def store(value_ref, out_ref, sem):
    copy = pltpu.make_async_copy(value_ref, out_ref, sem)
    copy.start()
    copy.wait()


def body(mesh, voltages, calib_gain, tile_flags, delays, pointing, synth_filter):
    nt, nz, nb = mesh.shape["tile"], mesh.shape["chan"], mesh.shape["beam"]
    total_rows, n_all = voltages.shape[:2]
    width = voltages.shape[-1]
    taps, k = synth_filter.shape
    tb = total_rows // nt
    fz = width // COARSE
    cz = COARSE // nz
    halo = -(-(taps - 1) // tb)
    n_own = calib_gain.shape[0]
    exchange = n_own % 4 == 0 and mesh.shape["beam"] > 1
    gain = calib_gain
    if not exchange:
        gain = gain * tile_flags.astype(F32)[:, None, None, None]
        gain = lax.all_gather(gain, "beam", axis=0, tiled=True)
    perm = gather_table(nz, fz, cz)
    dft = np.stack(dft_table(nz, fz)).reshape(2 * nz, 4, fz, 4 * k)
    cfg = (nt, nz, nb, tb, n_all, taps, fz, cz, halo, exchange)
    vmem = pl.BlockSpec(memory_space=pltpu.VMEM)
    anywhere = pl.BlockSpec(memory_space=pltpu.HBM)
    span = (halo + 1) * tb
    dma = pltpu.SemaphoreType.DMA
    pair = 2 if nt % 2 == 0 else 1
    chips = nt // pair
    reach = -(-(taps - 1) // (pair * tb))
    out = pl.pallas_call(
        functools.partial(kernel, cfg),
        out_shape=pltpu.VMEM((tb, cz, 2, 2 * k), F32),
        in_specs=[anywhere] * 8,
        out_specs=vmem,
        scratch_shapes=[
            pltpu.SMEM(tile_flags.shape, jnp.int32),
            pltpu.VMEM(delays.shape[::-1], F32),
            pltpu.SMEM(pointing.shape, jnp.int32),
            pltpu.VMEM(synth_filter.shape, F32),
            pltpu.VMEM(perm.shape, BF16),
            pltpu.VMEM(dft.shape, BF16),
            pltpu.VMEM((chips, cz, pair * tb * n_all * 4, LANES), BF16),
            pltpu.VMEM((cz, gain.shape[0] * 4, LANES), F32),
            pltpu.VMEM((nb, cz, n_own * 4, LANES), F32),
            pltpu.VMEM((cz, n_all * 4, LANES), F32),
            pltpu.VMEM((cz, n_all * 4, LANES), F32),
            pltpu.VMEM((chips, cz, pair * tb * 16, LANES), F32),
            pltpu.VMEM((chips, cz, 4, pair * tb, LANES), F32),
            pltpu.VMEM((nt - 1, cz, 4, pair * tb, LANES), F32),
            pltpu.VMEM((nz, cz, pair * tb, LANES), F32),
            pltpu.VMEM((nz, cz, span, LANES), F32),
            pltpu.VMEM((cz * span, 4 * k), F32),
            dma((5,)),
            dma((1,)),
            dma((cz,)),
            dma((1,)),
            dma((cz,)),
            dma((chips,)),
            dma((cz,)),
            dma((reach + 1, pair)),
            dma((reach + 1,)),
            dma((1,)),
        ],
        compiler_params=pltpu.CompilerParams(collective_id=0, has_side_effects=True),
    )(
        voltages.reshape(-1, 2, width),
        gain.reshape(-1, 2, width),
        tile_flags,
        delays.T,
        pointing,
        synth_filter,
        jnp.asarray(perm),
        jnp.asarray(dft),
    )
    final = pl.pallas_call(
        store,
        out_shape=jax.ShapeDtypeStruct(out.shape, F32),
        in_specs=[vmem],
        out_specs=pl.BlockSpec(memory_space=pltpu.HBM),
        scratch_shapes=[dma(())],
    )(pltpu.with_memory_space_constraint(out, pltpu.VMEM))
    return final.transpose(0, 2, 1, 3)[:, None]


def solution(mesh):
    in_specs = (
        P(None, "tile", None, None, "chan"),
        P(("tile", "beam"), None, None, "chan"),
        P(("tile", "beam")),
        P(None, "tile"),
        P("beam"),
        P(),
    )
    out_specs = P("tile", "beam", None, "chan", None)
    return jax.shard_map(
        functools.partial(body, mesh), mesh=mesh, in_specs=in_specs, out_specs=out_specs, check_vma=False
    )
```

```python
import functools
import math

import jax
import jax.numpy as jnp
import numpy as np
from jax import lax
from jax.experimental import pallas as pl
from jax.experimental.pallas import tpu as pltpu
from jax.sharding import PartitionSpec as P

COARSE = 12
LANES = 128
MESH = pl.DeviceIdType.MESH
F32 = jnp.float32
BF16 = jnp.bfloat16


def even_fit(func, degree):
    series = np.polynomial.chebyshev.Chebyshev.interpolate(
        lambda u: func(np.sqrt(u)), degree, domain=[0.0, 0.25]
    )
    return [float(v) for v in series.convert(kind=np.polynomial.Polynomial).coef]


COS_COEF = even_fit(lambda r: np.cos(2 * np.pi * r), 7)
SIN_COEF = even_fit(lambda r: 2 * np.pi * np.sinc(2 * r), 7)


def horner(coef, u):
    total = jnp.full_like(u, coef[-1])
    for value in coef[-2::-1]:
        total = total * u + value
    return total


def split_bf16(table):
    high = table.astype(BF16)
    low = (table - high.astype(np.float64)).astype(BF16)
    return high, low


def dft_table(nz, fz):
    k = nz * fz
    f = np.arange(k)
    m = np.arange(k)
    angle = 2 * np.pi * (f[:, None] * m[None, :] % k) / k
    cosine, sine = np.cos(angle) / math.sqrt(k), np.sin(angle) / math.sqrt(k)
    cosine, sine = cosine.reshape(nz // 2, 2, fz, k), sine.reshape(nz // 2, 2, fz, k)
    out = np.zeros((2, nz // 2, 2, 2, fz, 2, k))
    for p in range(2):
        for odd in range(2):
            place = odd ^ p
            out[p, :, place, 0, :, 0], out[p, :, place, 0, :, 1] = cosine[:, odd], sine[:, odd]
            out[p, :, place, 1, :, 0], out[p, :, place, 1, :, 1] = -sine[:, odd], cosine[:, odd]
    return split_bf16(out.reshape(nz, 4, fz, 2 * k))


def gather_table(nz, fz, cz):
    width = fz * COARSE
    out = np.zeros((width, width), np.float64)
    for c in range(cz):
        for z in range(nz):
            for f in range(fz):
                out[f * COARSE + z * cz + c, (c * nz + z) * fz + f] = 1.0
    return out.astype(BF16)


def kernel(
    cfg,
    volt_ref,
    gain_ref,
    flag_src,
    delay_src,
    point_src,
    synth_src,
    perm_src,
    dft_src,
    out_ref,
    flag_ref,
    delay_ref,
    point_ref,
    synth_ref,
    perm_ref,
    dft_ref,
    volt,
    own_gain,
    gains,
    w_re,
    w_im,
    acc,
    part,
    recv,
    packed,
    inbox,
    spec,
    gain_send,
    gain_recv,
    part_send,
    part_recv,
    pack_send,
    pack_recv,
):
    nt, nz, nb, tb, n_all, taps, fz, cz, halo, exchange = cfg
    tile = lax.axis_index("tile")
    chan = lax.axis_index("chan")
    beam = lax.axis_index("beam")
    rows_t = n_all * 4

    def peer(t, z, b):
        return {"tile": t, "chan": z, "beam": b}

    pair = 2 if nt % 2 == 0 else 1
    chips = nt // pair
    chip, core = lax.div(tile, pair), lax.rem(tile, pair)
    packer = pair - 1
    packs = core == packer
    order = sorted(range(1, chips), key=lambda a: abs(2 * a - chips)) + [0]
    block = pair * tb

    def chip_of(slot):
        return lax.rem(chip + order[slot], chips)

    def packer_of(target_chip):
        return target_chip * pair + packer

    span = (halo + 1) * tb

    def wait_all(ref, sem):
        pltpu.make_async_copy(ref, ref, sem).wait()

    reach = -(-(taps - 1) // block)

    def rows_of(back, k):
        shift = (halo - k) * tb - back * block
        low = max(0, halo * tb - (taps - 1) - shift)
        high = min(block, (halo + 1) * tb - shift)
        return low, max(high - low, 0), low + shift

    def early(small_sem, own_sem, volt_sem, dft_sem):
        gain_rows = gain_ref.reshape(gain_ref.shape[0] * 2, gain_ref.shape[2])
        for c in range(cz):
            pltpu.make_async_copy(
                gain_rows.at[:, pl.ds(c * LANES, LANES)], own_gain.at[c], own_sem.at[0]
            ).start()
        small = [
            pltpu.make_async_copy(src, dst, small_sem.at[i])
            for i, (src, dst) in enumerate(
                [
                    (flag_src, flag_ref),
                    (point_src, point_ref),
                    (delay_src, delay_ref),
                    (synth_src, synth_ref),
                    (perm_src, perm_ref),
                ]
            )
        ]
        dft_copies = [
            pltpu.make_async_copy(
                dft_src.at[:, g], dft_ref.at[:, lax.rem(chan + g, 4)], dft_sem.at[0]
            )
            for g in range(4)
        ]
        for copy in small[:3]:
            copy.start()

        barrier = pltpu.get_barrier_semaphore()

        def greet(t, z, b):
            pl.semaphore_signal(barrier, inc=1, device_id=peer(t, z, b), device_id_type=MESH)

        for db in range(1, nb):
            greet(tile, chan, lax.rem(beam + db, nb))
        if pair > 1:

            @pl.when(packs)
            def _():
                for a in range(chips):
                    for k in range(packer):
                        greet(lax.rem(chip + a, chips) * pair + k, chan, beam)

            @pl.when(jnp.logical_not(packs))
            def _():
                for a in range(chips):
                    greet(packer_of(lax.rem(chip + a, chips)), chan, beam)

        for dz in range(nz):
            for a in range(chips):
                if dz == 0:
                    if a:
                        pl.when(packs)(
                            functools.partial(greet, packer_of(lax.rem(chip + a, chips)), chan, beam)
                        )
                else:
                    greet(packer_of(lax.rem(chip + a, chips)), lax.rem(chan + dz, nz), beam)

        few = chips * (pair - 1) // max(packer, 1) + nb - 1
        many = nt * nz - 1 + nb - 1

        volt_rows = volt_ref.reshape(volt_ref.shape[0] * 2, volt_ref.shape[2])
        for c in range(cz):
            for slot in range(chips):
                pltpu.make_async_copy(
                    volt_rows.at[
                        pl.ds(chip_of(slot) * (block * rows_t), block * rows_t), pl.ds(c * LANES, LANES)
                    ],
                    volt.at[slot, c],
                    volt_sem.at[c],
                ).start()
        for copy in small[3:] + dft_copies:
            copy.start()

        row = lax.broadcasted_iota(jnp.int32, (8, LANES), 0)
        first = row < 4
        n_own = n_all // nb
        share = n_own * 4 if exchange else rows_t
        even = lax.rem(lax.broadcasted_iota(jnp.int32, (share, LANES), 0), 2) == 0

        with jax.named_scope("ownload"):
            wait_all(own_gain, own_sem.at[0])
            small[0].wait()
        if exchange:
            use = jnp.concatenate(
                [
                    jnp.where(first, flag_ref[2 * i].astype(F32), flag_ref[2 * i + 1].astype(F32))
                    for i in range(n_own // 2)
                ],
                axis=0,
            )
            for c in range(cz):
                gains[beam, c] = use * own_gain[c]

        unused = halo * tb - (taps - 1)
        if unused:
            inbox[:, :, pl.ds(0, unused), :] = jnp.zeros((nz, cz, unused, LANES), F32)
        for back in range(1, reach + 1):
            for k in range(pair):
                size, start = rows_of(back, k)[1:]
                if size:

                    @pl.when(jnp.logical_and(chip < back, core == k))
                    def _(size=size, start=start):
                        inbox[:, :, pl.ds(start, size), :] = jnp.zeros((nz, cz, size, LANES), F32)

        with jax.named_scope("barrier"):
            pl.semaphore_wait(barrier, few + core // max(packer, 1) * (many - few) if pair > 1 else many)

        if exchange:
            for c in range(cz):
                for db in range(1, nb):
                    pltpu.make_async_remote_copy(
                        src_ref=gains.at[beam, c],
                        dst_ref=gains.at[beam, c],
                        send_sem=gain_send.at[0],
                        recv_sem=gain_recv.at[c],
                        device_id=peer(tile, chan, lax.rem(beam + db, nb)),
                        device_id_type=MESH,
                    ).start()

        for copy in small[1:3]:
            copy.wait()
        select = lax.broadcasted_iota(jnp.int32, delay_ref.shape, 1) == point_ref[0]
        delay = jnp.sum(jnp.where(select, delay_ref[...], 0.0), axis=1, keepdims=True)
        delay = jnp.broadcast_to(delay, (n_all, LANES))
        delay = jnp.concatenate(
            [
                jnp.where(
                    first,
                    jnp.broadcast_to(delay[2 * i : 2 * i + 1], (8, LANES)),
                    jnp.broadcast_to(delay[2 * i + 1 : 2 * i + 2], (8, LANES)),
                )
                for i in range(n_all // 2)
            ],
            axis=0,
        )
        for c in range(cz):
            local = (lax.broadcasted_iota(jnp.int32, (1, LANES), 1) + c * LANES).astype(F32)
            fine = jnp.floor((local + 0.5) / COARSE)
            channel = (local - COARSE * fine) * (nz * fz) + fine + (chan * fz).astype(F32)
            frequency = (channel + 0.5) / (COARSE * nz * fz)
            cycles = delay * frequency
            turn = cycles - jnp.floor(cycles + 0.5)
            square = turn * turn
            w_re[c] = horner(COS_COEF, square)
            w_im[c] = turn * horner(SIN_COEF, square)

        def weigh(c, start, gain):
            rows = pl.ds(start, share)
            swapped = jnp.where(even, pltpu.roll(gain, share - 1, 0), -pltpu.roll(gain, 1, 0))
            weight = gain * w_re[c, rows, :] + swapped * w_im[c, rows, :]
            w_re[c, rows, :] = jnp.where(even, weight, pltpu.roll(weight, 1, 0))
            w_im[c, rows, :] = jnp.where(even, pltpu.roll(weight, share - 1, 0), weight)

        unroll = math.gcd(block, 8)

        def accumulate(slot, c, starts, extend):
            def step(s, carry):
                sums = [[jnp.zeros((16, LANES), F32)] * 2 for _ in range(unroll)]
                for start in starts:
                    for q in range(share // 16):
                        at = start + q * 16
                        wr = w_re[c, pl.ds(at, 16), :]
                        wi = w_im[c, pl.ds(at, 16), :]
                        for u in range(unroll):
                            begin = pl.multiple_of((s * unroll + u) * rows_t + at, 16)
                            v = volt[slot, c, pl.ds(begin, 16), :].astype(F32)
                            sums[u] = [sums[u][0] + wr * v, sums[u][1] + wi * v]
                for u in range(unroll):
                    begin = pl.multiple_of((s * unroll + u) * 16, 16)
                    for which in range(2):
                        value = sums[u][which]
                        value = value[:8] + value[8:]
                        rows = pl.ds(begin + which * 8, 8)
                        acc[slot, c, rows, :] = acc[slot, c, rows, :] + value if extend else value
                return carry

            lax.fori_loop(0, block // unroll, step, 0)

        def take(slot, c, which, p, ri):
            total = None
            for half in range(2):
                value = acc[slot, c, pl.ds(which * 8 + half * 4 + p * 2 + ri, block, stride=16), :]
                total = value if total is None else total + value
            return total

        starts = [0]
        if exchange:
            starts = [pl.multiple_of(lax.rem(beam + db, nb) * share, 16) for db in range(nb)]
        with jax.named_scope("acc1"):
            for c in range(cz):
                weigh(c, starts[0], gains[beam, c] if exchange else own_gain[c])
                if exchange:
                    wait_all(volt.at[:, c], volt_sem.at[c])

                    def first_sum(slot, carry, c=c):
                        accumulate(slot, c, starts[:1], False)
                        return carry

                    lax.fori_loop(0, chips, first_sum, 0)
        for c in range(cz):
            with jax.named_scope(f"gainwait{c}"):
                if exchange:
                    wait_all(gains.at[pl.ds(0, nb - 1), c], gain_recv.at[c])
                else:
                    wait_all(volt.at[:, c], volt_sem.at[c])
            for db in range(1, nb if exchange else 1):
                weigh(c, starts[db], gains[lax.rem(beam + db, nb), c])
            for slot in range(chips):
                if exchange:
                    accumulate(slot, c, starts[1:], True)
                else:
                    accumulate(slot, c, starts, False)
                for p in range(2):
                    part[slot, c, p * 2] = take(slot, c, 0, p, 0) - take(slot, c, 1, p, 1)
                    part[slot, c, p * 2 + 1] = take(slot, c, 0, p, 1) + take(slot, c, 1, p, 0)
                def send(slot=slot, c=c):
                    pltpu.make_async_remote_copy(
                        src_ref=part.at[slot, c],
                        dst_ref=recv.at[slot * pair + core, c],
                        send_sem=part_send.at[slot],
                        recv_sem=part_recv.at[c],
                        device_id=peer(packer_of(chip_of(slot)), chan, beam),
                        device_id_type=MESH,
                    ).start()

                if slot < chips - 1:
                    send()
                elif pair > 1:
                    pl.when(jnp.logical_not(packs))(send)

        half = 2 * chan // nz
        place = chan * half + (nz - 1 - chan) * (1 - half)

        def target(i):
            if i == nz - 1:
                return chan
            other = i + (i + nz - place) // nz
            return other * half + (nz - 1 - other) * (1 - half)

        for copy in small[3:]:
            copy.wait()

        @pl.when(packs)
        def _():
            moved = jnp.zeros((4 * block, cz * LANES), F32)
            for c in range(cz):
                with jax.named_scope(f"partwait{c}"):
                    wait_all(recv.at[:, c], part_recv.at[c])
                sums = part[chips - 1, c]
                for i in range(nt - 1):
                    sums = sums + recv[i, c]
                sums = sums.reshape(4 * block, LANES)
                high = sums.astype(BF16)
                low = (sums - high.astype(F32)).astype(BF16)
                table = perm_ref[pl.ds(c * LANES, LANES), :]
                both = jnp.dot(
                    jnp.concatenate([high, low], axis=0), table, preferred_element_type=F32
                )
                moved = moved + both[: 4 * block] + both[4 * block :]
            group = lax.broadcasted_iota(jnp.int32, (block, LANES), 1) // fz
            quarter = 2 * lax.rem(chan, 2)
            turned = [
                [
                    pltpu.roll(
                        moved[g * block : (g + 1) * block, c * LANES : (c + 1) * LANES],
                        lax.rem(quarter + g, 4) * fz,
                        1,
                    )
                    for g in range(4)
                ]
                for c in range(cz)
            ]
            for i in range(nz):
                z = target(i)
                for c in range(cz):
                    total = turned[c][0]
                    for g in range(1, 4):
                        total = jnp.where(group == lax.rem(quarter + g + z, 4), turned[c][g], total)
                    packed[z, c] = total
            messages = sorted(
                (i + (0.5 if k == packer else 2.5) * (back > 0), i, back, k)
                for i in range(nz)
                for back in range(reach + 1)
                for k in range(pair)
                if rows_of(back, k)[1] and (i < nz - 1 or back or k < packer)
            )
            for _, i, back, k in messages:
                begin, size, start = rows_of(back, k)

                def send(i=i, back=back, k=k, begin=begin, size=size, start=start):
                    pltpu.make_async_remote_copy(
                        src_ref=packed.at[target(i), :, pl.ds(begin, size), :],
                        dst_ref=inbox.at[chan, :, pl.ds(start, size), :],
                        send_sem=pack_send.at[back, k],
                        recv_sem=pack_recv.at[back],
                        device_id=peer(lax.rem(chip + back, chips) * pair + k, target(i), beam),
                        device_id_type=MESH,
                    ).start()

                if back == 0:
                    send()
                else:
                    pl.when(chip + back < chips)(send)

            begin, size, start = rows_of(0, packer)
            inbox[chan, :, pl.ds(start, size), :] = packed[chan, :, pl.ds(begin, size), :]

        for copy in dft_copies:
            copy.wait()

    dma = pltpu.SemaphoreType.DMA
    pl.run_scoped(early, dma((5,)), dma((1,)), dma((cz,)), dma((1,)))

    def each_group(sends):
        for back in range(reach + 1):
            for k in range(pair):
                begin, size, start = rows_of(back, k)
                if not size:
                    continue
                count = nz - 1 if back == 0 and k == packer else nz
                there = packs if sends else core == k
                if back:
                    there = jnp.logical_and(there, chip + back < chips if sends else chip >= back)

                @pl.when(there)
                def _(back=back, k=k, count=count, begin=begin, size=size, start=start):
                    if sends:
                        wait_all(packed.at[pl.ds(0, count), :, pl.ds(begin, size), :], pack_send.at[back, k])
                    else:
                        wait_all(inbox.at[pl.ds(0, count), :, pl.ds(start, size), :], pack_recv.at[back])

    with jax.named_scope("packwait"):
        each_group(False)

    lane = lax.broadcasted_iota(jnp.int32, (span, LANES), 1) // fz
    early_half = lax.rem(lane + 4 - lax.rem(chan, 4), 4) < 2
    for p in range(2):
        lhs = jnp.concatenate(
            [
                jnp.concatenate(
                    [
                        jnp.where(early_half, inbox[2 * j + p, c], inbox[2 * j + 1 - p, c])
                        for j in range(nz // 2)
                    ],
                    axis=1,
                )
                for c in range(cz)
            ],
            axis=0,
        )
        high = lhs.astype(BF16)
        low = (lhs - high.astype(F32)).astype(BF16)
        dft_h, dft_l = [
            dft_ref[pl.ds(at + p * (nz // 2), nz // 2)].reshape(nz // 2 * 4 * fz, 2 * nz * fz)
            for at in (0, nz)
        ]
        both = jnp.dot(jnp.concatenate([high, low], axis=0), dft_h, preferred_element_type=F32)
        spec[p] = (
            both[: cz * span]
            + both[cz * span :]
            + jnp.dot(high, dft_l, preferred_element_type=F32)
        )
    for c in range(cz):
        for g in range(4):
            total = None
            for k in range(taps):
                value = synth_ref[pl.ds(k, 1), :] * spec[
                    g // 2, pl.ds(c * span + halo * tb - k, tb), g % 2 * LANES : (g % 2 + 1) * LANES
                ]
                total = value if total is None else total + value
            for t in range(tb):
                out_ref[t, c, pl.ds(g // 2, 1), (g % 2) * LANES : (g % 2 + 1) * LANES] = total[t : t + 1]

    with jax.named_scope("sendwait"):
        if exchange:
            wait_all(gains.at[pl.ds(0, nb - 1)], gain_send.at[0])
        for slot in range(chips):
            if slot < chips - 1:
                wait_all(part.at[slot], part_send.at[slot])
            elif pair > 1:

                @pl.when(jnp.logical_not(packs))
                def _():
                    wait_all(part.at[chips - 1], part_send.at[chips - 1])

        each_group(True)


def store(value_ref, out_ref, sem):
    copy = pltpu.make_async_copy(value_ref, out_ref, sem)
    copy.start()
    copy.wait()


def body(mesh, voltages, calib_gain, tile_flags, delays, pointing, synth_filter):
    nt, nz, nb = mesh.shape["tile"], mesh.shape["chan"], mesh.shape["beam"]
    total_rows, n_all = voltages.shape[:2]
    width = voltages.shape[-1]
    taps, k = synth_filter.shape
    tb = total_rows // nt
    fz = width // COARSE
    cz = COARSE // nz
    halo = -(-(taps - 1) // tb)
    n_own = calib_gain.shape[0]
    exchange = n_own % 4 == 0 and mesh.shape["beam"] > 1
    gain = calib_gain
    if not exchange:
        gain = gain * tile_flags.astype(F32)[:, None, None, None]
        gain = lax.all_gather(gain, "beam", axis=0, tiled=True)
    perm = gather_table(nz, fz, cz)
    dft = np.concatenate(dft_table(nz, fz))
    cfg = (nt, nz, nb, tb, n_all, taps, fz, cz, halo, exchange)
    vmem = pl.BlockSpec(memory_space=pltpu.VMEM)
    anywhere = pl.BlockSpec(memory_space=pltpu.HBM)
    span = (halo + 1) * tb
    dma = pltpu.SemaphoreType.DMA
    pair = 2 if nt % 2 == 0 else 1
    chips = nt // pair
    reach = -(-(taps - 1) // (pair * tb))
    out = pl.pallas_call(
        functools.partial(kernel, cfg),
        out_shape=pltpu.VMEM((tb, cz, 2, 2 * k), F32),
        in_specs=[anywhere] * 8,
        out_specs=vmem,
        scratch_shapes=[
            pltpu.SMEM(tile_flags.shape, jnp.int32),
            pltpu.VMEM(delays.shape[::-1], F32),
            pltpu.SMEM(pointing.shape, jnp.int32),
            pltpu.VMEM(synth_filter.shape, F32),
            pltpu.VMEM(perm.shape, BF16),
            pltpu.VMEM(dft.shape, BF16),
            pltpu.VMEM((chips, cz, pair * tb * n_all * 4, LANES), BF16),
            pltpu.VMEM((cz, gain.shape[0] * 4, LANES), F32),
            pltpu.VMEM((nb, cz, n_own * 4, LANES), F32),
            pltpu.VMEM((cz, n_all * 4, LANES), F32),
            pltpu.VMEM((cz, n_all * 4, LANES), F32),
            pltpu.VMEM((chips, cz, pair * tb * 16, LANES), F32),
            pltpu.VMEM((chips, cz, 4, pair * tb, LANES), F32),
            pltpu.VMEM((nt - 1, cz, 4, pair * tb, LANES), F32),
            pltpu.VMEM((nz, cz, pair * tb, LANES), F32),
            pltpu.VMEM((nz, cz, span, LANES), F32),
            pltpu.VMEM((2, cz * span, 2 * k), F32),
            dma((1,)),
            dma((cz,)),
            dma((chips,)),
            dma((cz,)),
            dma((reach + 1, pair)),
            dma((reach + 1,)),
        ],
        compiler_params=pltpu.CompilerParams(collective_id=0, has_side_effects=True),
    )(
        voltages.reshape(-1, 2, width),
        gain.reshape(-1, 2, width),
        tile_flags,
        delays.T,
        pointing,
        synth_filter,
        jnp.asarray(perm),
        jnp.asarray(dft),
    )
    final = pl.pallas_call(
        store,
        out_shape=jax.ShapeDtypeStruct(out.shape, F32),
        in_specs=[vmem],
        out_specs=pl.BlockSpec(memory_space=pltpu.HBM),
        scratch_shapes=[dma(())],
    )(pltpu.with_memory_space_constraint(out, pltpu.VMEM))
    return final.transpose(0, 2, 1, 3)[:, None]


def solution(mesh):
    in_specs = (
        P(None, "tile", None, None, "chan"),
        P(("tile", "beam"), None, None, "chan"),
        P(("tile", "beam")),
        P(None, "tile"),
        P("beam"),
        P(),
    )
    out_specs = P("tile", "beam", None, "chan", None)
    return jax.shard_map(
        functools.partial(body, mesh), mesh=mesh, in_specs=in_specs, out_specs=out_specs, check_vma=False
    )
```

```python
import functools
import math

import jax
import jax.numpy as jnp
import numpy as np
from jax import lax
from jax.experimental import pallas as pl
from jax.experimental.pallas import tpu as pltpu
from jax.sharding import PartitionSpec as P

COARSE = 12
LANES = 128
MESH = pl.DeviceIdType.MESH
F32 = jnp.float32
BF16 = jnp.bfloat16


def even_fit(func, degree):
    series = np.polynomial.chebyshev.Chebyshev.interpolate(
        lambda u: func(np.sqrt(u)), degree, domain=[0.0, 0.25]
    )
    return [float(v) for v in series.convert(kind=np.polynomial.Polynomial).coef]


COS_COEF = even_fit(lambda r: np.cos(2 * np.pi * r), 7)
SIN_COEF = even_fit(lambda r: 2 * np.pi * np.sinc(2 * r), 7)


def horner(coef, u):
    total = jnp.full_like(u, coef[-1])
    for value in coef[-2::-1]:
        total = total * u + value
    return total


def split_bf16(table):
    high = table.astype(BF16)
    low = (table - high.astype(np.float64)).astype(BF16)
    return high, low


def dft_table(nz, fz):
    k = nz * fz
    f = np.arange(k)
    m = np.arange(k)
    angle = 2 * np.pi * (f[:, None] * m[None, :] % k) / k
    cosine, sine = np.cos(angle) / math.sqrt(k), np.sin(angle) / math.sqrt(k)
    cosine, sine = cosine.reshape(nz // 2, 2, fz, k), sine.reshape(nz // 2, 2, fz, k)
    out = np.zeros((2, nz // 2, 2, 2, fz, 2, k))
    for p in range(2):
        for odd in range(2):
            place = odd ^ p
            out[p, :, place, 0, :, 0], out[p, :, place, 0, :, 1] = cosine[:, odd], sine[:, odd]
            out[p, :, place, 1, :, 0], out[p, :, place, 1, :, 1] = -sine[:, odd], cosine[:, odd]
    return split_bf16(out.reshape(nz, 4, fz, 2 * k))


def gather_table(nz, fz, cz):
    width = fz * COARSE
    out = np.zeros((width, width), np.float64)
    for c in range(cz):
        for z in range(nz):
            for f in range(fz):
                out[f * COARSE + z * cz + c, (c * nz + z) * fz + f] = 1.0
    return out.astype(BF16)


def kernel(
    cfg,
    volt_ref,
    gain_ref,
    flag_src,
    delay_src,
    point_src,
    synth_src,
    perm_src,
    dft_src,
    out_ref,
    flag_ref,
    delay_ref,
    point_ref,
    synth_ref,
    perm_ref,
    dft_ref,
    volt,
    own_gain,
    gains,
    w_re,
    w_im,
    acc,
    part,
    recv,
    packed,
    inbox,
    spec,
    gain_send,
    gain_recv,
    part_send,
    part_recv,
    pack_send,
    pack_recv,
    ready,
):
    nt, nz, nb, tb, n_all, taps, fz, cz, halo, exchange = cfg
    tile = lax.axis_index("tile")
    chan = lax.axis_index("chan")
    beam = lax.axis_index("beam")
    rows_t = n_all * 4

    def peer(t, z, b):
        return {"tile": t, "chan": z, "beam": b}

    pair = 2 if nt % 2 == 0 else 1
    chips = nt // pair
    chip, core = lax.div(tile, pair), lax.rem(tile, pair)
    packer = pair - 1
    packs = core == packer
    order = sorted(range(1, chips), key=lambda a: abs(2 * a - chips)) + [0]
    block = pair * tb

    def chip_of(slot):
        return lax.rem(chip + order[slot], chips)

    def packer_of(target_chip):
        return target_chip * pair + packer

    span = (halo + 1) * tb

    def wait_all(ref, sem):
        pltpu.make_async_copy(ref, ref, sem).wait()

    reach = -(-(taps - 1) // block)

    def rows_of(back, k):
        shift = (halo - k) * tb - back * block
        low = max(0, halo * tb - (taps - 1) - shift)
        high = min(block, (halo + 1) * tb - shift)
        return low, max(high - low, 0), low + shift

    def early(small_sem, own_sem, volt_sem, dft_sem):
        gain_rows = gain_ref.reshape(gain_ref.shape[0] * 2, gain_ref.shape[2])
        for c in range(cz):
            pltpu.make_async_copy(
                gain_rows.at[:, pl.ds(c * LANES, LANES)], own_gain.at[c], own_sem.at[0]
            ).start()
        small = [
            pltpu.make_async_copy(src, dst, small_sem.at[i])
            for i, (src, dst) in enumerate(
                [
                    (flag_src, flag_ref),
                    (point_src, point_ref),
                    (delay_src, delay_ref),
                    (synth_src, synth_ref),
                    (perm_src, perm_ref),
                ]
            )
        ]
        dft_copies = [
            pltpu.make_async_copy(
                dft_src.at[:, g], dft_ref.at[:, lax.rem(chan + g, 4)], dft_sem.at[0]
            )
            for g in range(4)
        ]
        for copy in small[:3]:
            copy.start()

        barrier = pltpu.get_barrier_semaphore()

        def greet(t, z, b):
            pl.semaphore_signal(barrier, inc=1, device_id=peer(t, z, b), device_id_type=MESH)

        for db in range(1, nb):
            greet(chip * pair, chan, lax.rem(beam + db, nb))
            if pair > 1:
                pl.when(packs)(functools.partial(greet, tile, chan, lax.rem(beam + db, nb)))
        if pair > 1:

            @pl.when(packs)
            def _():
                for a in range(chips):
                    for k in range(packer):
                        greet(lax.rem(chip + a, chips) * pair + k, chan, beam)

            @pl.when(jnp.logical_not(packs))
            def _():
                for a in range(chips):
                    greet(packer_of(lax.rem(chip + a, chips)), chan, beam)

        for dz in range(nz):
            for a in range(chips):
                if dz == 0:
                    if a:
                        pl.when(packs)(
                            functools.partial(greet, packer_of(lax.rem(chip + a, chips)), chan, beam)
                        )
                else:
                    greet(packer_of(lax.rem(chip + a, chips)), lax.rem(chan + dz, nz), beam)

        volt_rows = volt_ref.reshape(volt_ref.shape[0] * 2, volt_ref.shape[2])
        for c in range(cz):
            for slot in range(chips):
                pltpu.make_async_copy(
                    volt_rows.at[
                        pl.ds(chip_of(slot) * (block * rows_t), block * rows_t), pl.ds(c * LANES, LANES)
                    ],
                    volt.at[slot, c],
                    volt_sem.at[c],
                ).start()
        for copy in small[3:] + dft_copies:
            copy.start()

        row = lax.broadcasted_iota(jnp.int32, (8, LANES), 0)
        first = row < 4
        n_own = n_all // nb
        share = n_own * 4 if exchange else rows_t
        even = lax.rem(lax.broadcasted_iota(jnp.int32, (share, LANES), 0), 2) == 0

        with jax.named_scope("ownload"):
            wait_all(own_gain, own_sem.at[0])
            small[0].wait()
        if exchange:
            use = jnp.concatenate(
                [
                    jnp.where(first, flag_ref[2 * i].astype(F32), flag_ref[2 * i + 1].astype(F32))
                    for i in range(n_own // 2)
                ],
                axis=0,
            )
            for c in range(cz):
                gains[beam, c] = use * own_gain[c]

        unused = halo * tb - (taps - 1)
        if unused:
            inbox[:, :, pl.ds(0, unused), :] = jnp.zeros((nz, cz, unused, LANES), F32)
        for back in range(1, reach + 1):
            for k in range(pair):
                size, start = rows_of(back, k)[1:]
                if size:

                    @pl.when(jnp.logical_and(chip < back, core == k))
                    def _(size=size, start=start):
                        inbox[:, :, pl.ds(start, size), :] = jnp.zeros((nz, cz, size, LANES), F32)

        with jax.named_scope("barrier"):
            if pair > 1:

                @pl.when(jnp.logical_not(packs))
                def _():
                    pl.semaphore_wait(barrier, chips + (nb - 1) * pair)
                    pl.semaphore_signal(
                        ready,
                        inc=1,
                        device_id=peer(packer_of(chip), chan, beam),
                        device_id_type=MESH,
                    )

                @pl.when(jnp.logical_and(packs, chan < nz - 1))
                def _():
                    pl.semaphore_wait(ready, 1)

                @pl.when(jnp.logical_and(packs, chan == nz - 1))
                def _():
                    pl.semaphore_wait(barrier, nt * nz - 1 + nb - 1)

            else:
                pl.semaphore_wait(barrier, nt * nz - 1 + nb - 1)

        if exchange:
            for c in range(cz):
                for db in range(1, nb):
                    pltpu.make_async_remote_copy(
                        src_ref=gains.at[beam, c],
                        dst_ref=gains.at[beam, c],
                        send_sem=gain_send.at[0],
                        recv_sem=gain_recv.at[c],
                        device_id=peer(tile, chan, lax.rem(beam + db, nb)),
                        device_id_type=MESH,
                    ).start()

        for copy in small[1:3]:
            copy.wait()
        select = lax.broadcasted_iota(jnp.int32, delay_ref.shape, 1) == point_ref[0]
        delay = jnp.sum(jnp.where(select, delay_ref[...], 0.0), axis=1, keepdims=True)
        delay = jnp.broadcast_to(delay, (n_all, LANES))
        delay = jnp.concatenate(
            [
                jnp.where(
                    first,
                    jnp.broadcast_to(delay[2 * i : 2 * i + 1], (8, LANES)),
                    jnp.broadcast_to(delay[2 * i + 1 : 2 * i + 2], (8, LANES)),
                )
                for i in range(n_all // 2)
            ],
            axis=0,
        )
        for c in range(cz):
            local = (lax.broadcasted_iota(jnp.int32, (1, LANES), 1) + c * LANES).astype(F32)
            fine = jnp.floor((local + 0.5) / COARSE)
            channel = (local - COARSE * fine) * (nz * fz) + fine + (chan * fz).astype(F32)
            frequency = (channel + 0.5) / (COARSE * nz * fz)
            cycles = delay * frequency
            turn = cycles - jnp.floor(cycles + 0.5)
            square = turn * turn
            w_re[c] = horner(COS_COEF, square)
            w_im[c] = turn * horner(SIN_COEF, square)

        def weigh(c, start, gain):
            rows = pl.ds(start, share)
            swapped = jnp.where(even, pltpu.roll(gain, share - 1, 0), -pltpu.roll(gain, 1, 0))
            weight = gain * w_re[c, rows, :] + swapped * w_im[c, rows, :]
            w_re[c, rows, :] = jnp.where(even, weight, pltpu.roll(weight, 1, 0))
            w_im[c, rows, :] = jnp.where(even, pltpu.roll(weight, share - 1, 0), weight)

        unroll = math.gcd(block, 8)

        def accumulate(slot, c, starts, extend):
            def step(s, carry):
                sums = [[jnp.zeros((16, LANES), F32)] * 2 for _ in range(unroll)]
                for start in starts:
                    for q in range(share // 16):
                        at = start + q * 16
                        wr = w_re[c, pl.ds(at, 16), :]
                        wi = w_im[c, pl.ds(at, 16), :]
                        for u in range(unroll):
                            begin = pl.multiple_of((s * unroll + u) * rows_t + at, 16)
                            v = volt[slot, c, pl.ds(begin, 16), :].astype(F32)
                            sums[u] = [sums[u][0] + wr * v, sums[u][1] + wi * v]
                for u in range(unroll):
                    begin = pl.multiple_of((s * unroll + u) * 16, 16)
                    for which in range(2):
                        value = sums[u][which]
                        value = value[:8] + value[8:]
                        rows = pl.ds(begin + which * 8, 8)
                        acc[slot, c, rows, :] = acc[slot, c, rows, :] + value if extend else value
                return carry

            lax.fori_loop(0, block // unroll, step, 0)

        def take(slot, c, which, p, ri):
            total = None
            for half in range(2):
                value = acc[slot, c, pl.ds(which * 8 + half * 4 + p * 2 + ri, block, stride=16), :]
                total = value if total is None else total + value
            return total

        starts = [0]
        if exchange:
            starts = [pl.multiple_of(lax.rem(beam + db, nb) * share, 16) for db in range(nb)]
        with jax.named_scope("acc1"):
            for c in range(cz):
                weigh(c, starts[0], gains[beam, c] if exchange else own_gain[c])
                if exchange:
                    wait_all(volt.at[:, c], volt_sem.at[c])

                    def first_sum(slot, carry, c=c):
                        accumulate(slot, c, starts[:1], False)
                        return carry

                    lax.fori_loop(0, chips, first_sum, 0)
        if pair > 1:

            @pl.when(jnp.logical_and(packs, chan < nz - 1))
            def _():
                with jax.named_scope("barrier2"):
                    pl.semaphore_wait(barrier, nt * nz - 1 + nb - 1)

            @pl.when(jnp.logical_and(packs, chan == nz - 1))
            def _():
                pl.semaphore_wait(ready, 1)

        for c in range(cz):
            with jax.named_scope(f"gainwait{c}"):
                if exchange:
                    wait_all(gains.at[pl.ds(0, nb - 1), c], gain_recv.at[c])
                else:
                    wait_all(volt.at[:, c], volt_sem.at[c])
            for db in range(1, nb if exchange else 1):
                weigh(c, starts[db], gains[lax.rem(beam + db, nb), c])
            for slot in range(chips):
                if exchange:
                    accumulate(slot, c, starts[1:], True)
                else:
                    accumulate(slot, c, starts, False)
                for p in range(2):
                    part[slot, c, p * 2] = take(slot, c, 0, p, 0) - take(slot, c, 1, p, 1)
                    part[slot, c, p * 2 + 1] = take(slot, c, 0, p, 1) + take(slot, c, 1, p, 0)
                def send(slot=slot, c=c):
                    pltpu.make_async_remote_copy(
                        src_ref=part.at[slot, c],
                        dst_ref=recv.at[slot * pair + core, c],
                        send_sem=part_send.at[slot],
                        recv_sem=part_recv.at[c],
                        device_id=peer(packer_of(chip_of(slot)), chan, beam),
                        device_id_type=MESH,
                    ).start()

                if slot < chips - 1:
                    send()
                elif pair > 1:
                    pl.when(jnp.logical_not(packs))(send)

        half = 2 * chan // nz
        place = chan * half + (nz - 1 - chan) * (1 - half)

        def target(i):
            if i == nz - 1:
                return chan
            other = i + (i + nz - place) // nz
            return other * half + (nz - 1 - other) * (1 - half)

        for copy in small[3:]:
            copy.wait()

        @pl.when(packs)
        def _():
            moved = jnp.zeros((4 * block, cz * LANES), F32)
            for c in range(cz):
                with jax.named_scope(f"partwait{c}"):
                    wait_all(recv.at[:, c], part_recv.at[c])
                sums = part[chips - 1, c]
                for i in range(nt - 1):
                    sums = sums + recv[i, c]
                sums = sums.reshape(4 * block, LANES)
                high = sums.astype(BF16)
                low = (sums - high.astype(F32)).astype(BF16)
                table = perm_ref[pl.ds(c * LANES, LANES), :]
                both = jnp.dot(
                    jnp.concatenate([high, low], axis=0), table, preferred_element_type=F32
                )
                moved = moved + both[: 4 * block] + both[4 * block :]
            group = lax.broadcasted_iota(jnp.int32, (block, LANES), 1) // fz
            quarter = 2 * lax.rem(chan, 2)
            turned = [
                [
                    pltpu.roll(
                        moved[g * block : (g + 1) * block, c * LANES : (c + 1) * LANES],
                        lax.rem(quarter + g, 4) * fz,
                        1,
                    )
                    for g in range(4)
                ]
                for c in range(cz)
            ]
            for i in range(nz):
                z = target(i)
                for c in range(cz):
                    total = turned[c][0]
                    for g in range(1, 4):
                        total = jnp.where(group == lax.rem(quarter + g + z, 4), turned[c][g], total)
                    packed[z, c] = total
            messages = sorted(
                (i + (0.5 if k == packer else 0.6) * (back > 0), i, back, k)
                for i in range(nz)
                for back in range(reach + 1)
                for k in range(pair)
                if rows_of(back, k)[1] and (i < nz - 1 or back or k < packer)
            )
            for _, i, back, k in messages:
                begin, size, start = rows_of(back, k)

                def send(i=i, back=back, k=k, begin=begin, size=size, start=start):
                    pltpu.make_async_remote_copy(
                        src_ref=packed.at[target(i), :, pl.ds(begin, size), :],
                        dst_ref=inbox.at[chan, :, pl.ds(start, size), :],
                        send_sem=pack_send.at[back, k],
                        recv_sem=pack_recv.at[back],
                        device_id=peer(lax.rem(chip + back, chips) * pair + k, target(i), beam),
                        device_id_type=MESH,
                    ).start()

                if back == 0:
                    send()
                else:
                    pl.when(chip + back < chips)(send)

            begin, size, start = rows_of(0, packer)
            inbox[chan, :, pl.ds(start, size), :] = packed[chan, :, pl.ds(begin, size), :]

        for copy in dft_copies:
            copy.wait()

    dma = pltpu.SemaphoreType.DMA
    pl.run_scoped(early, dma((5,)), dma((1,)), dma((cz,)), dma((1,)))

    def each_group(sends):
        for back in range(reach + 1):
            for k in range(pair):
                begin, size, start = rows_of(back, k)
                if not size:
                    continue
                count = nz - 1 if back == 0 and k == packer else nz
                there = packs if sends else core == k
                if back:
                    there = jnp.logical_and(there, chip + back < chips if sends else chip >= back)

                @pl.when(there)
                def _(back=back, k=k, count=count, begin=begin, size=size, start=start):
                    if sends:
                        wait_all(packed.at[pl.ds(0, count), :, pl.ds(begin, size), :], pack_send.at[back, k])
                    else:
                        wait_all(inbox.at[pl.ds(0, count), :, pl.ds(start, size), :], pack_recv.at[back])

    with jax.named_scope("packwait"):
        each_group(False)

    lane = lax.broadcasted_iota(jnp.int32, (span, LANES), 1) // fz
    early_half = lax.rem(lane + 4 - lax.rem(chan, 4), 4) < 2
    for p in range(2):
        lhs = jnp.concatenate(
            [
                jnp.concatenate(
                    [
                        jnp.where(early_half, inbox[2 * j + p, c], inbox[2 * j + 1 - p, c])
                        for j in range(nz // 2)
                    ],
                    axis=1,
                )
                for c in range(cz)
            ],
            axis=0,
        )
        high = lhs.astype(BF16)
        low = (lhs - high.astype(F32)).astype(BF16)
        dft_h, dft_l = [
            dft_ref[pl.ds(at + p * (nz // 2), nz // 2)].reshape(nz // 2 * 4 * fz, 2 * nz * fz)
            for at in (0, nz)
        ]
        both = jnp.dot(jnp.concatenate([high, low], axis=0), dft_h, preferred_element_type=F32)
        spec[p] = (
            both[: cz * span]
            + both[cz * span :]
            + jnp.dot(high, dft_l, preferred_element_type=F32)
        )
    for c in range(cz):
        for g in range(4):
            total = None
            for k in range(taps):
                value = synth_ref[pl.ds(k, 1), :] * spec[
                    g // 2, pl.ds(c * span + halo * tb - k, tb), g % 2 * LANES : (g % 2 + 1) * LANES
                ]
                total = value if total is None else total + value
            for t in range(tb):
                out_ref[t, c, pl.ds(g // 2, 1), (g % 2) * LANES : (g % 2 + 1) * LANES] = total[t : t + 1]

    with jax.named_scope("sendwait"):
        if exchange:
            wait_all(gains.at[pl.ds(0, nb - 1)], gain_send.at[0])
        for slot in range(chips):
            if slot < chips - 1:
                wait_all(part.at[slot], part_send.at[slot])
            elif pair > 1:

                @pl.when(jnp.logical_not(packs))
                def _():
                    wait_all(part.at[chips - 1], part_send.at[chips - 1])

        each_group(True)


def store(value_ref, out_ref, sem):
    copy = pltpu.make_async_copy(value_ref, out_ref, sem)
    copy.start()
    copy.wait()


def body(mesh, voltages, calib_gain, tile_flags, delays, pointing, synth_filter):
    nt, nz, nb = mesh.shape["tile"], mesh.shape["chan"], mesh.shape["beam"]
    total_rows, n_all = voltages.shape[:2]
    width = voltages.shape[-1]
    taps, k = synth_filter.shape
    tb = total_rows // nt
    fz = width // COARSE
    cz = COARSE // nz
    halo = -(-(taps - 1) // tb)
    n_own = calib_gain.shape[0]
    exchange = n_own % 4 == 0 and mesh.shape["beam"] > 1
    gain = calib_gain
    if not exchange:
        gain = gain * tile_flags.astype(F32)[:, None, None, None]
        gain = lax.all_gather(gain, "beam", axis=0, tiled=True)
    perm = gather_table(nz, fz, cz)
    dft = np.concatenate(dft_table(nz, fz))
    cfg = (nt, nz, nb, tb, n_all, taps, fz, cz, halo, exchange)
    vmem = pl.BlockSpec(memory_space=pltpu.VMEM)
    anywhere = pl.BlockSpec(memory_space=pltpu.HBM)
    span = (halo + 1) * tb
    dma = pltpu.SemaphoreType.DMA
    pair = 2 if nt % 2 == 0 else 1
    chips = nt // pair
    reach = -(-(taps - 1) // (pair * tb))
    out = pl.pallas_call(
        functools.partial(kernel, cfg),
        out_shape=pltpu.VMEM((tb, cz, 2, 2 * k), F32),
        in_specs=[anywhere] * 8,
        out_specs=vmem,
        scratch_shapes=[
            pltpu.SMEM(tile_flags.shape, jnp.int32),
            pltpu.VMEM(delays.shape[::-1], F32),
            pltpu.SMEM(pointing.shape, jnp.int32),
            pltpu.VMEM(synth_filter.shape, F32),
            pltpu.VMEM(perm.shape, BF16),
            pltpu.VMEM(dft.shape, BF16),
            pltpu.VMEM((chips, cz, pair * tb * n_all * 4, LANES), BF16),
            pltpu.VMEM((cz, gain.shape[0] * 4, LANES), F32),
            pltpu.VMEM((nb, cz, n_own * 4, LANES), F32),
            pltpu.VMEM((cz, n_all * 4, LANES), F32),
            pltpu.VMEM((cz, n_all * 4, LANES), F32),
            pltpu.VMEM((chips, cz, pair * tb * 16, LANES), F32),
            pltpu.VMEM((chips, cz, 4, pair * tb, LANES), F32),
            pltpu.VMEM((nt - 1, cz, 4, pair * tb, LANES), F32),
            pltpu.VMEM((nz, cz, pair * tb, LANES), F32),
            pltpu.VMEM((nz, cz, span, LANES), F32),
            pltpu.VMEM((2, cz * span, 2 * k), F32),
            dma((1,)),
            dma((cz,)),
            dma((chips,)),
            dma((cz,)),
            dma((reach + 1, pair)),
            dma((reach + 1,)),
            pltpu.SemaphoreType.REGULAR,
        ],
        compiler_params=pltpu.CompilerParams(collective_id=0, has_side_effects=True),
    )(
        voltages.reshape(-1, 2, width),
        gain.reshape(-1, 2, width),
        tile_flags,
        delays.T,
        pointing,
        synth_filter,
        jnp.asarray(perm),
        jnp.asarray(dft),
    )
    final = pl.pallas_call(
        store,
        out_shape=jax.ShapeDtypeStruct(out.shape, F32),
        in_specs=[vmem],
        out_specs=pl.BlockSpec(memory_space=pltpu.HBM),
        scratch_shapes=[dma(())],
    )(pltpu.with_memory_space_constraint(out, pltpu.VMEM))
    return final.transpose(0, 2, 1, 3)[:, None]


def solution(mesh):
    in_specs = (
        P(None, "tile", None, None, "chan"),
        P(("tile", "beam"), None, None, "chan"),
        P(("tile", "beam")),
        P(None, "tile"),
        P("beam"),
        P(),
    )
    out_specs = P("tile", "beam", None, "chan", None)
    return jax.shard_map(
        functools.partial(body, mesh), mesh=mesh, in_specs=in_specs, out_specs=out_specs, check_vma=False
    )
```

```python
import functools
import math

import jax
import jax.numpy as jnp
import numpy as np
from jax import lax
from jax.experimental import pallas as pl
from jax.experimental.pallas import tpu as pltpu
from jax.sharding import PartitionSpec as P

COARSE = 12
LANES = 128
MESH = pl.DeviceIdType.MESH
F32 = jnp.float32
BF16 = jnp.bfloat16


def even_fit(func, degree):
    series = np.polynomial.chebyshev.Chebyshev.interpolate(
        lambda u: func(np.sqrt(u)), degree, domain=[0.0, 0.25]
    )
    return [float(v) for v in series.convert(kind=np.polynomial.Polynomial).coef]


COS_COEF = even_fit(lambda r: np.cos(2 * np.pi * r), 7)
SIN_COEF = even_fit(lambda r: 2 * np.pi * np.sinc(2 * r), 7)


def horner(coef, u):
    total = jnp.full_like(u, coef[-1])
    for value in coef[-2::-1]:
        total = total * u + value
    return total


def split_bf16(table):
    high = table.astype(BF16)
    low = (table - high.astype(np.float64)).astype(BF16)
    return high, low


def dft_table(nz, fz):
    k = nz * fz
    f = np.arange(k)
    m = np.arange(k)
    angle = 2 * np.pi * (f[:, None] * m[None, :] % k) / k
    cosine, sine = np.cos(angle) / math.sqrt(k), np.sin(angle) / math.sqrt(k)
    cosine, sine = cosine.reshape(nz // 2, 2, fz, k), sine.reshape(nz // 2, 2, fz, k)
    out = np.zeros((2, nz // 2, 2, 2, fz, 2, k))
    for p in range(2):
        for odd in range(2):
            place = odd ^ p
            out[p, :, place, 0, :, 0], out[p, :, place, 0, :, 1] = cosine[:, odd], sine[:, odd]
            out[p, :, place, 1, :, 0], out[p, :, place, 1, :, 1] = -sine[:, odd], cosine[:, odd]
    return split_bf16(out.reshape(nz, 4, fz, 2 * k))


def gather_table(nz, fz, cz):
    width = fz * COARSE
    out = np.zeros((width, width), np.float64)
    for c in range(cz):
        for z in range(nz):
            for f in range(fz):
                out[f * COARSE + z * cz + c, (c * nz + z) * fz + f] = 1.0
    return out.astype(BF16)


def kernel(
    cfg,
    volt_ref,
    gain_ref,
    flag_src,
    delay_src,
    point_src,
    synth_src,
    perm_src,
    dft_src,
    out_ref,
    flag_ref,
    delay_ref,
    point_ref,
    synth_ref,
    perm_ref,
    dft_ref,
    volt,
    own_gain,
    gains,
    w_re,
    w_im,
    acc,
    part,
    recv,
    packed,
    inbox,
    spec,
    send_sem,
    gain_recv,
    part_recv,
    pack_recv,
    ready,
):
    nt, nz, nb, tb, n_all, taps, fz, cz, halo, exchange = cfg
    tile = lax.axis_index("tile")
    chan = lax.axis_index("chan")
    beam = lax.axis_index("beam")
    rows_t = n_all * 4

    def peer(t, z, b):
        return {"tile": t, "chan": z, "beam": b}

    pair = 2 if nt % 2 == 0 else 1
    chips = nt // pair
    chip, core = lax.div(tile, pair), lax.rem(tile, pair)
    packer = pair - 1
    packs = core == packer
    order = sorted(range(1, chips), key=lambda a: abs(2 * a - chips)) + [0]
    block = pair * tb

    def chip_of(slot):
        return lax.rem(chip + order[slot], chips)

    def packer_of(target_chip):
        return target_chip * pair + packer

    span = (halo + 1) * tb

    def wait_all(ref, sem):
        pltpu.make_async_copy(ref, ref, sem).wait()

    reach = -(-(taps - 1) // block)
    n_own = n_all // nb
    share = n_own * 4 if exchange else rows_t

    def rows_of(back, k):
        shift = (halo - k) * tb - back * block
        low = max(0, halo * tb - (taps - 1) - shift)
        high = min(block, (halo + 1) * tb - shift)
        return low, max(high - low, 0), low + shift

    def early(small_sem, own_sem, volt_sem, dft_sem):
        gain_rows = gain_ref.reshape(gain_ref.shape[0] * 2, gain_ref.shape[2])
        for c in range(cz):
            pltpu.make_async_copy(
                gain_rows.at[:, pl.ds(c * LANES, LANES)], own_gain.at[c], own_sem.at[0]
            ).start()
        small = [
            pltpu.make_async_copy(src, dst, small_sem.at[i])
            for i, (src, dst) in enumerate(
                [
                    (flag_src, flag_ref),
                    (point_src, point_ref),
                    (delay_src, delay_ref),
                    (synth_src, synth_ref),
                    (perm_src, perm_ref),
                ]
            )
        ]
        dft_copies = [
            pltpu.make_async_copy(
                dft_src.at[:, g], dft_ref.at[:, lax.rem(chan + g, 4)], dft_sem.at[0]
            )
            for g in range(4)
        ]
        for copy in small[:3]:
            copy.start()

        barrier = pltpu.get_barrier_semaphore()

        def greet(t, z, b):
            pl.semaphore_signal(barrier, inc=1, device_id=peer(t, z, b), device_id_type=MESH)

        for db in range(1, nb):
            greet(chip * pair, chan, lax.rem(beam + db, nb))
            if pair > 1:
                pl.when(packs)(functools.partial(greet, tile, chan, lax.rem(beam + db, nb)))
        if pair > 1:

            @pl.when(packs)
            def _():
                for a in range(chips):
                    for k in range(packer):
                        greet(lax.rem(chip + a, chips) * pair + k, chan, beam)

            @pl.when(jnp.logical_not(packs))
            def _():
                for a in range(chips):
                    greet(packer_of(lax.rem(chip + a, chips)), chan, beam)

        for dz in range(nz):
            for a in range(chips):
                if dz == 0:
                    if a:
                        pl.when(packs)(
                            functools.partial(greet, packer_of(lax.rem(chip + a, chips)), chan, beam)
                        )
                else:
                    greet(packer_of(lax.rem(chip + a, chips)), lax.rem(chan + dz, nz), beam)

        volt_rows = volt_ref.reshape(volt_ref.shape[0] * 2, volt_ref.shape[2])
        for c in range(cz):
            for slot in range(chips):
                pltpu.make_async_copy(
                    volt_rows.at[
                        pl.ds(chip_of(slot) * (block * rows_t), block * rows_t), pl.ds(c * LANES, LANES)
                    ],
                    volt.at[slot, c],
                    volt_sem.at[c],
                ).start()
        for copy in small[3:] + dft_copies:
            copy.start()

        row = lax.broadcasted_iota(jnp.int32, (8, LANES), 0)
        first = row < 4
        even = lax.rem(lax.broadcasted_iota(jnp.int32, (share, LANES), 0), 2) == 0

        with jax.named_scope("ownload"):
            wait_all(own_gain, own_sem.at[0])
            small[0].wait()
        if exchange:
            use = jnp.concatenate(
                [
                    jnp.where(first, flag_ref[2 * i].astype(F32), flag_ref[2 * i + 1].astype(F32))
                    for i in range(n_own // 2)
                ],
                axis=0,
            )
            for c in range(cz):
                gains[beam, c] = use * own_gain[c]

        unused = halo * tb - (taps - 1)
        if unused:
            inbox[:, :, pl.ds(0, unused), :] = jnp.zeros((nz, cz, unused, LANES), F32)
        for back in range(1, reach + 1):
            for k in range(pair):
                size, start = rows_of(back, k)[1:]
                if size:

                    @pl.when(jnp.logical_and(chip < back, core == k))
                    def _(size=size, start=start):
                        inbox[:, :, pl.ds(start, size), :] = jnp.zeros((nz, cz, size, LANES), F32)

        with jax.named_scope("barrier"):
            if pair > 1:

                @pl.when(jnp.logical_not(packs))
                def _():
                    pl.semaphore_wait(barrier, chips + (nb - 1) * pair)
                    pl.semaphore_signal(
                        ready,
                        inc=1,
                        device_id=peer(packer_of(chip), chan, beam),
                        device_id_type=MESH,
                    )

                @pl.when(jnp.logical_and(packs, chan < nz - 1))
                def _():
                    pl.semaphore_wait(ready, 1)

                @pl.when(jnp.logical_and(packs, chan == nz - 1))
                def _():
                    pl.semaphore_wait(barrier, nt * nz - 1 + nb - 1)

            else:
                pl.semaphore_wait(barrier, nt * nz - 1 + nb - 1)

        if exchange:
            for c in range(cz):
                for db in range(1, nb):
                    pltpu.make_async_remote_copy(
                        src_ref=gains.at[beam, c],
                        dst_ref=gains.at[beam, c],
                        send_sem=send_sem.at[0],
                        recv_sem=gain_recv.at[c],
                        device_id=peer(tile, chan, lax.rem(beam + db, nb)),
                        device_id_type=MESH,
                    ).start()

        for copy in small[1:3]:
            copy.wait()
        select = lax.broadcasted_iota(jnp.int32, delay_ref.shape, 1) == point_ref[0]
        delay = jnp.sum(jnp.where(select, delay_ref[...], 0.0), axis=1, keepdims=True)
        delay = jnp.broadcast_to(delay, (n_all, LANES))
        delay = jnp.concatenate(
            [
                jnp.where(
                    first,
                    jnp.broadcast_to(delay[2 * i : 2 * i + 1], (8, LANES)),
                    jnp.broadcast_to(delay[2 * i + 1 : 2 * i + 2], (8, LANES)),
                )
                for i in range(n_all // 2)
            ],
            axis=0,
        )
        for c in range(cz):
            local = (lax.broadcasted_iota(jnp.int32, (1, LANES), 1) + c * LANES).astype(F32)
            fine = jnp.floor((local + 0.5) / COARSE)
            channel = (local - COARSE * fine) * (nz * fz) + fine + (chan * fz).astype(F32)
            frequency = (channel + 0.5) / (COARSE * nz * fz)
            cycles = delay * frequency
            turn = cycles - jnp.floor(cycles + 0.5)
            square = turn * turn
            w_re[c] = horner(COS_COEF, square)
            w_im[c] = turn * horner(SIN_COEF, square)

        def weigh(c, start, gain):
            rows = pl.ds(start, share)
            swapped = jnp.where(even, pltpu.roll(gain, share - 1, 0), -pltpu.roll(gain, 1, 0))
            weight = gain * w_re[c, rows, :] + swapped * w_im[c, rows, :]
            w_re[c, rows, :] = jnp.where(even, weight, pltpu.roll(weight, 1, 0))
            w_im[c, rows, :] = jnp.where(even, pltpu.roll(weight, share - 1, 0), weight)

        unroll = math.gcd(block, 8)

        def accumulate(slot, c, starts, extend):
            def step(s, carry):
                sums = [[jnp.zeros((16, LANES), F32)] * 2 for _ in range(unroll)]
                for start in starts:
                    for q in range(share // 16):
                        at = start + q * 16
                        wr = w_re[c, pl.ds(at, 16), :]
                        wi = w_im[c, pl.ds(at, 16), :]
                        for u in range(unroll):
                            begin = pl.multiple_of((s * unroll + u) * rows_t + at, 16)
                            v = volt[slot, c, pl.ds(begin, 16), :].astype(F32)
                            sums[u] = [sums[u][0] + wr * v, sums[u][1] + wi * v]
                for u in range(unroll):
                    begin = pl.multiple_of((s * unroll + u) * 16, 16)
                    for which in range(2):
                        value = sums[u][which]
                        value = value[:8] + value[8:]
                        rows = pl.ds(begin + which * 8, 8)
                        acc[slot, c, rows, :] = acc[slot, c, rows, :] + value if extend else value
                return carry

            lax.fori_loop(0, block // unroll, step, 0)

        def take(slot, c, which, p, ri):
            total = None
            for half in range(2):
                value = acc[slot, c, pl.ds(which * 8 + half * 4 + p * 2 + ri, block, stride=16), :]
                total = value if total is None else total + value
            return total

        starts = [0]
        if exchange:
            starts = [pl.multiple_of(lax.rem(beam + db, nb) * share, 16) for db in range(nb)]
        with jax.named_scope("acc1"):
            for c in range(cz):
                weigh(c, starts[0], gains[beam, c] if exchange else own_gain[c])
                if exchange:
                    wait_all(volt.at[:, c], volt_sem.at[c])

                    def first_sum(slot, carry, c=c):
                        accumulate(slot, c, starts[:1], False)
                        return carry

                    lax.fori_loop(0, chips, first_sum, 0)
        if pair > 1:

            @pl.when(jnp.logical_and(packs, chan < nz - 1))
            def _():
                with jax.named_scope("barrier2"):
                    pl.semaphore_wait(barrier, nt * nz - 1 + nb - 1)

            @pl.when(jnp.logical_and(packs, chan == nz - 1))
            def _():
                pl.semaphore_wait(ready, 1)

        for c in range(cz):
            with jax.named_scope(f"gainwait{c}"):
                if exchange:
                    wait_all(gains.at[pl.ds(0, nb - 1), c], gain_recv.at[c])
                else:
                    wait_all(volt.at[:, c], volt_sem.at[c])
            for db in range(1, nb if exchange else 1):
                weigh(c, starts[db], gains[lax.rem(beam + db, nb), c])
            for slot in range(chips):
                if exchange:
                    accumulate(slot, c, starts[1:], True)
                else:
                    accumulate(slot, c, starts, False)
                for p in range(2):
                    part[slot, c, p * 2] = take(slot, c, 0, p, 0) - take(slot, c, 1, p, 1)
                    part[slot, c, p * 2 + 1] = take(slot, c, 0, p, 1) + take(slot, c, 1, p, 0)
                def send(slot=slot, c=c):
                    pltpu.make_async_remote_copy(
                        src_ref=part.at[slot, c],
                        dst_ref=recv.at[slot * pair + core, c],
                        send_sem=send_sem.at[0],
                        recv_sem=part_recv.at[c],
                        device_id=peer(packer_of(chip_of(slot)), chan, beam),
                        device_id_type=MESH,
                    ).start()

                if slot < chips - 1:
                    send()
                elif pair > 1:
                    pl.when(jnp.logical_not(packs))(send)

        half = 2 * chan // nz
        place = chan * half + (nz - 1 - chan) * (1 - half)

        def target(i):
            if i == nz - 1:
                return chan
            other = i + (i + nz - place) // nz
            return other * half + (nz - 1 - other) * (1 - half)

        for copy in small[3:]:
            copy.wait()

        @pl.when(packs)
        def _():
            moved = jnp.zeros((4 * block, cz * LANES), F32)
            for c in range(cz):
                with jax.named_scope(f"partwait{c}"):
                    wait_all(recv.at[:, c], part_recv.at[c])
                sums = part[chips - 1, c]
                for i in range(nt - 1):
                    sums = sums + recv[i, c]
                sums = sums.reshape(4 * block, LANES)
                high = sums.astype(BF16)
                low = (sums - high.astype(F32)).astype(BF16)
                table = perm_ref[pl.ds(c * LANES, LANES), :]
                both = jnp.dot(
                    jnp.concatenate([high, low], axis=0), table, preferred_element_type=F32
                )
                moved = moved + both[: 4 * block] + both[4 * block :]
            group = lax.broadcasted_iota(jnp.int32, (block, LANES), 1) // fz
            quarter = 2 * lax.rem(chan, 2)
            turned = [
                [
                    pltpu.roll(
                        moved[g * block : (g + 1) * block, c * LANES : (c + 1) * LANES],
                        lax.rem(quarter + g, 4) * fz,
                        1,
                    )
                    for g in range(4)
                ]
                for c in range(cz)
            ]
            for i in range(nz):
                z = target(i)
                for c in range(cz):
                    total = turned[c][0]
                    for g in range(1, 4):
                        total = jnp.where(group == lax.rem(quarter + g + z, 4), turned[c][g], total)
                    packed[z, c] = total
                for back in range(reach + 1):
                    for k in range(pair) if back == 0 else range(pair - 1, -1, -1):
                        begin, size, start = rows_of(back, k)
                        if not size or (i == nz - 1 and back == 0 and k == packer):
                            continue

                        def send(i=i, back=back, k=k, begin=begin, size=size, start=start):
                            pltpu.make_async_remote_copy(
                                src_ref=packed.at[target(i), :, pl.ds(begin, size), :],
                                dst_ref=inbox.at[chan, :, pl.ds(start, size), :],
                                send_sem=send_sem.at[0],
                                recv_sem=pack_recv.at[back],
                                device_id=peer(lax.rem(chip + back, chips) * pair + k, target(i), beam),
                                device_id_type=MESH,
                            ).start()

                        if back == 0:
                            send()
                        else:
                            pl.when(chip + back < chips)(send)

            begin, size, start = rows_of(0, packer)
            inbox[chan, :, pl.ds(start, size), :] = packed[chan, :, pl.ds(begin, size), :]

        for copy in dft_copies:
            copy.wait()

    dma = pltpu.SemaphoreType.DMA
    pl.run_scoped(early, dma((5,)), dma((1,)), dma((cz,)), dma((1,)))

    def sent_rows(packing, reached):
        rows = (nb - 1) * cz * share if exchange else 0
        rows += (chips - packing) * cz * 4 * block
        if packing:
            for back in range(reached + 1):
                for k in range(pair):
                    count = nz - 1 if back == 0 and k == packer else nz
                    rows += count * cz * rows_of(back, k)[1]
        return rows

    def wait_sent(packing, reached):
        flat = acc.reshape(chips * cz * block * 16, LANES)
        wait_all(flat.at[pl.ds(0, sent_rows(packing, reached)), :], send_sem.at[0])

    with jax.named_scope("packwait"):
        for back in range(reach + 1):
            for k in range(pair):
                size, start = rows_of(back, k)[1:]
                if not size:
                    continue
                count = nz - 1 if back == 0 and k == packer else nz

                @pl.when(jnp.logical_and(core == k, chip >= back))
                def _(back=back, count=count, size=size, start=start):
                    wait_all(inbox.at[pl.ds(0, count), :, pl.ds(start, size), :], pack_recv.at[back])

    lane = lax.broadcasted_iota(jnp.int32, (span, LANES), 1) // fz
    early_half = lax.rem(lane + 4 - lax.rem(chan, 4), 4) < 2
    for p in range(2):
        lhs = jnp.concatenate(
            [
                jnp.concatenate(
                    [
                        jnp.where(early_half, inbox[2 * j + p, c], inbox[2 * j + 1 - p, c])
                        for j in range(nz // 2)
                    ],
                    axis=1,
                )
                for c in range(cz)
            ],
            axis=0,
        )
        high = lhs.astype(BF16)
        low = (lhs - high.astype(F32)).astype(BF16)
        dft_h, dft_l = [
            dft_ref[pl.ds(at + p * (nz // 2), nz // 2)].reshape(nz // 2 * 4 * fz, 2 * nz * fz)
            for at in (0, nz)
        ]
        both = jnp.dot(jnp.concatenate([high, low], axis=0), dft_h, preferred_element_type=F32)
        value = (
            both[: cz * span]
            + both[cz * span :]
            + jnp.dot(high, dft_l, preferred_element_type=F32)
        )
        for ri in range(2):
            spec[p * 2 + ri] = value[:, ri * LANES : (ri + 1) * LANES]
    for c in range(cz):
        for g in range(4):
            total = None
            for k in range(taps):
                value = synth_ref[pl.ds(k, 1), :] * spec[
                    g, pl.ds(c * span + halo * tb - k, tb), :
                ]
                total = value if total is None else total + value
            for t in range(tb):
                out_ref[t, c, pl.ds(g // 2, 1), (g % 2) * LANES : (g % 2 + 1) * LANES] = total[t : t + 1]

    with jax.named_scope("sendwait"):
        if pair > 1:
            pl.when(jnp.logical_not(packs))(functools.partial(wait_sent, 0, 0))
        for reached in range(min(reach, chips - 1) + 1):
            above = chips - 1 - chip
            here = above >= reach if reached == reach else above == reached
            pl.when(jnp.logical_and(packs, here))(functools.partial(wait_sent, 1, reached))


def store(value_ref, out_ref, sem):
    copy = pltpu.make_async_copy(value_ref, out_ref, sem)
    copy.start()
    copy.wait()


def body(mesh, voltages, calib_gain, tile_flags, delays, pointing, synth_filter):
    nt, nz, nb = mesh.shape["tile"], mesh.shape["chan"], mesh.shape["beam"]
    total_rows, n_all = voltages.shape[:2]
    width = voltages.shape[-1]
    taps, k = synth_filter.shape
    tb = total_rows // nt
    fz = width // COARSE
    cz = COARSE // nz
    halo = -(-(taps - 1) // tb)
    n_own = calib_gain.shape[0]
    exchange = n_own % 4 == 0 and mesh.shape["beam"] > 1
    gain = calib_gain
    if not exchange:
        gain = gain * tile_flags.astype(F32)[:, None, None, None]
        gain = lax.all_gather(gain, "beam", axis=0, tiled=True)
    perm = gather_table(nz, fz, cz)
    dft = np.concatenate(dft_table(nz, fz))
    cfg = (nt, nz, nb, tb, n_all, taps, fz, cz, halo, exchange)
    vmem = pl.BlockSpec(memory_space=pltpu.VMEM)
    anywhere = pl.BlockSpec(memory_space=pltpu.HBM)
    span = (halo + 1) * tb
    dma = pltpu.SemaphoreType.DMA
    pair = 2 if nt % 2 == 0 else 1
    chips = nt // pair
    reach = -(-(taps - 1) // (pair * tb))
    out = pl.pallas_call(
        functools.partial(kernel, cfg),
        out_shape=pltpu.VMEM((tb, cz, 2, 2 * k), F32),
        in_specs=[anywhere] * 8,
        out_specs=vmem,
        scratch_shapes=[
            pltpu.SMEM(tile_flags.shape, jnp.int32),
            pltpu.VMEM(delays.shape[::-1], F32),
            pltpu.SMEM(pointing.shape, jnp.int32),
            pltpu.VMEM(synth_filter.shape, F32),
            pltpu.VMEM(perm.shape, BF16),
            pltpu.VMEM(dft.shape, BF16),
            pltpu.VMEM((chips, cz, pair * tb * n_all * 4, LANES), BF16),
            pltpu.VMEM((cz, gain.shape[0] * 4, LANES), F32),
            pltpu.VMEM((nb, cz, n_own * 4, LANES), F32),
            pltpu.VMEM((cz, n_all * 4, LANES), F32),
            pltpu.VMEM((cz, n_all * 4, LANES), F32),
            pltpu.VMEM((chips, cz, pair * tb * 16, LANES), F32),
            pltpu.VMEM((chips, cz, 4, pair * tb, LANES), F32),
            pltpu.VMEM((nt - 1, cz, 4, pair * tb, LANES), F32),
            pltpu.VMEM((nz, cz, pair * tb, LANES), F32),
            pltpu.VMEM((nz, cz, span, LANES), F32),
            pltpu.VMEM((4, cz * span, k), F32),
            dma((1,)),
            dma((cz,)),
            dma((cz,)),
            dma((reach + 1,)),
            pltpu.SemaphoreType.REGULAR,
        ],
        compiler_params=pltpu.CompilerParams(collective_id=0, has_side_effects=True),
    )(
        voltages.reshape(-1, 2, width),
        gain.reshape(-1, 2, width),
        tile_flags,
        delays.T,
        pointing,
        synth_filter,
        jnp.asarray(perm),
        jnp.asarray(dft),
    )
    final = pl.pallas_call(
        store,
        out_shape=jax.ShapeDtypeStruct(out.shape, F32),
        in_specs=[vmem],
        out_specs=pl.BlockSpec(memory_space=pltpu.HBM),
        scratch_shapes=[dma(())],
    )(pltpu.with_memory_space_constraint(out, pltpu.VMEM))
    return final.transpose(0, 2, 1, 3)[:, None]


def solution(mesh):
    in_specs = (
        P(None, "tile", None, None, "chan"),
        P(("tile", "beam"), None, None, "chan"),
        P(("tile", "beam")),
        P(None, "tile"),
        P("beam"),
        P(),
    )
    out_specs = P("tile", "beam", None, "chan", None)
    return jax.shard_map(
        functools.partial(body, mesh), mesh=mesh, in_specs=in_specs, out_specs=out_specs, check_vma=False
    )
```

```python
import functools
import math

import jax
import jax.numpy as jnp
import numpy as np
from jax import lax
from jax.experimental import pallas as pl
from jax.experimental.pallas import tpu as pltpu
from jax.sharding import PartitionSpec as P

COARSE = 12
LANES = 128
MESH = pl.DeviceIdType.MESH
F32 = jnp.float32
BF16 = jnp.bfloat16


def even_fit(func, degree):
    series = np.polynomial.chebyshev.Chebyshev.interpolate(
        lambda u: func(np.sqrt(u)), degree, domain=[0.0, 0.25]
    )
    return [float(v) for v in series.convert(kind=np.polynomial.Polynomial).coef]


COS_COEF = even_fit(lambda r: np.cos(2 * np.pi * r), 7)
SIN_COEF = even_fit(lambda r: 2 * np.pi * np.sinc(2 * r), 7)


def horner(coef, u):
    total = jnp.full_like(u, coef[-1])
    for value in coef[-2::-1]:
        total = total * u + value
    return total


def split_bf16(table):
    high = table.astype(BF16)
    low = (table - high.astype(np.float64)).astype(BF16)
    return high, low


def dft_table(nz, fz):
    k = nz * fz
    f = np.arange(k)
    m = np.arange(k)
    angle = 2 * np.pi * (f[:, None] * m[None, :] % k) / k
    cosine, sine = np.cos(angle) / math.sqrt(k), np.sin(angle) / math.sqrt(k)
    cosine, sine = cosine.reshape(nz // 2, 2, fz, k), sine.reshape(nz // 2, 2, fz, k)
    out = np.zeros((2, nz // 2, 2, 2, fz, 2, k))
    for p in range(2):
        for odd in range(2):
            place = odd ^ p
            out[p, :, place, 0, :, 0], out[p, :, place, 0, :, 1] = cosine[:, odd], sine[:, odd]
            out[p, :, place, 1, :, 0], out[p, :, place, 1, :, 1] = -sine[:, odd], cosine[:, odd]
    return split_bf16(out.reshape(nz, 4, fz, 2 * k))


def gather_table(nz, fz, cz):
    width = fz * COARSE
    out = np.zeros((width, width), np.float64)
    for c in range(cz):
        for z in range(nz):
            for f in range(fz):
                out[f * COARSE + z * cz + c, (c * nz + z) * fz + f] = 1.0
    return out.astype(BF16)


def kernel(
    cfg,
    volt_ref,
    gain_ref,
    flag_src,
    delay_src,
    point_src,
    synth_src,
    perm_src,
    dft_src,
    out_ref,
    flag_ref,
    delay_ref,
    point_ref,
    synth_ref,
    perm_ref,
    dft_ref,
    volt,
    own_gain,
    gains,
    w_re,
    w_im,
    acc,
    part,
    recv,
    packed,
    inbox,
    spec,
    send_sem,
    gain_recv,
    part_recv,
    pack_recv,
    ready,
):
    nt, nz, nb, tb, n_all, taps, fz, cz, halo, exchange = cfg
    tile = lax.axis_index("tile")
    chan = lax.axis_index("chan")
    beam = lax.axis_index("beam")
    rows_t = n_all * 4

    def peer(t, z, b):
        return {"tile": t, "chan": z, "beam": b}

    pair = 2 if nt % 2 == 0 else 1
    chips = nt // pair
    chip, core = lax.div(tile, pair), lax.rem(tile, pair)
    packer = pair - 1
    packs = core == packer
    order = sorted(range(1, chips), key=lambda a: abs(2 * a - chips)) + [0]
    block = pair * tb

    def chip_of(slot):
        return lax.rem(chip + order[slot], chips)

    def packer_of(target_chip):
        return target_chip * pair + packer

    span = (halo + 1) * tb

    def wait_all(ref, sem):
        pltpu.make_async_copy(ref, ref, sem).wait()

    reach = -(-(taps - 1) // block)
    n_own = n_all // nb
    share = n_own * 4 if exchange else rows_t

    def rows_of(back, k):
        shift = (halo - k) * tb - back * block
        low = max(0, halo * tb - (taps - 1) - shift)
        high = min(block, (halo + 1) * tb - shift)
        return low, max(high - low, 0), low + shift

    def early(small_sem, own_sem, volt_sem, dft_sem):
        gain_rows = gain_ref.reshape(gain_ref.shape[0] * 2, gain_ref.shape[2])
        for c in range(cz):
            pltpu.make_async_copy(
                gain_rows.at[:, pl.ds(c * LANES, LANES)], own_gain.at[c], own_sem.at[0]
            ).start()
        small = [
            pltpu.make_async_copy(src, dst, small_sem.at[i])
            for i, (src, dst) in enumerate(
                [
                    (flag_src, flag_ref),
                    (point_src, point_ref),
                    (delay_src, delay_ref),
                    (synth_src, synth_ref),
                    (perm_src, perm_ref),
                ]
            )
        ]
        dft_copies = [
            pltpu.make_async_copy(
                dft_src.at[:, g], dft_ref.at[:, lax.rem(chan + g, 4)], dft_sem.at[0]
            )
            for g in range(4)
        ]
        for copy in small[:3]:
            copy.start()

        barrier = pltpu.get_barrier_semaphore()

        def greet(t, z, b):
            pl.semaphore_signal(barrier, inc=1, device_id=peer(t, z, b), device_id_type=MESH)

        for db in range(1, nb):
            greet(chip * pair, chan, lax.rem(beam + db, nb))
            if pair > 1:
                pl.when(packs)(functools.partial(greet, tile, chan, lax.rem(beam + db, nb)))
        if pair > 1:

            @pl.when(packs)
            def _():
                for a in range(chips):
                    for k in range(packer):
                        greet(lax.rem(chip + a, chips) * pair + k, chan, beam)

            @pl.when(jnp.logical_not(packs))
            def _():
                for a in range(chips):
                    greet(packer_of(lax.rem(chip + a, chips)), chan, beam)

        for dz in range(nz):
            for a in range(chips):
                if dz == 0:
                    if a:
                        pl.when(packs)(
                            functools.partial(greet, packer_of(lax.rem(chip + a, chips)), chan, beam)
                        )
                else:
                    greet(packer_of(lax.rem(chip + a, chips)), lax.rem(chan + dz, nz), beam)

        volt_rows = volt_ref.reshape(volt_ref.shape[0] * 2, volt_ref.shape[2])
        for c in range(cz):
            for slot in range(chips):
                pltpu.make_async_copy(
                    volt_rows.at[
                        pl.ds(chip_of(slot) * (block * rows_t), block * rows_t), pl.ds(c * LANES, LANES)
                    ],
                    volt.at[slot, c],
                    volt_sem.at[c],
                ).start()
        for copy in small[3:] + dft_copies:
            copy.start()

        row = lax.broadcasted_iota(jnp.int32, (8, LANES), 0)
        first = row < 4
        even = lax.rem(lax.broadcasted_iota(jnp.int32, (share, LANES), 0), 2) == 0

        with jax.named_scope("ownload"):
            wait_all(own_gain, own_sem.at[0])
            small[0].wait()
        if exchange:
            use = jnp.concatenate(
                [
                    jnp.where(first, flag_ref[2 * i].astype(F32), flag_ref[2 * i + 1].astype(F32))
                    for i in range(n_own // 2)
                ],
                axis=0,
            )
            for c in range(cz):
                gains[beam, c] = use * own_gain[c]

        unused = halo * tb - (taps - 1)
        if unused:
            inbox[:, :, pl.ds(0, unused), :] = jnp.zeros((nz, cz, unused, LANES), F32)
        for back in range(1, reach + 1):
            for k in range(pair):
                size, start = rows_of(back, k)[1:]
                if size:

                    @pl.when(jnp.logical_and(chip < back, core == k))
                    def _(size=size, start=start):
                        inbox[:, :, pl.ds(start, size), :] = jnp.zeros((nz, cz, size, LANES), F32)

        with jax.named_scope("barrier"):
            if pair > 1:

                @pl.when(jnp.logical_not(packs))
                def _():
                    pl.semaphore_wait(barrier, chips + (nb - 1) * pair)
                    pl.semaphore_signal(
                        ready,
                        inc=1,
                        device_id=peer(packer_of(chip), chan, beam),
                        device_id_type=MESH,
                    )

                @pl.when(jnp.logical_and(packs, chan < nz - 1))
                def _():
                    pl.semaphore_wait(ready, 1)

                @pl.when(jnp.logical_and(packs, chan == nz - 1))
                def _():
                    pl.semaphore_wait(barrier, nt * nz - 1 + nb - 1)

            else:
                pl.semaphore_wait(barrier, nt * nz - 1 + nb - 1)

        if exchange:
            for c in range(cz):
                for db in range(1, nb):
                    pltpu.make_async_remote_copy(
                        src_ref=gains.at[beam, c],
                        dst_ref=gains.at[beam, c],
                        send_sem=send_sem.at[0],
                        recv_sem=gain_recv.at[c],
                        device_id=peer(tile, chan, lax.rem(beam + db, nb)),
                        device_id_type=MESH,
                    ).start()

        for copy in small[1:3]:
            copy.wait()
        select = lax.broadcasted_iota(jnp.int32, delay_ref.shape, 1) == point_ref[0]
        delay = jnp.sum(jnp.where(select, delay_ref[...], 0.0), axis=1, keepdims=True)
        delay = jnp.broadcast_to(delay, (n_all, LANES))
        delay = jnp.concatenate(
            [
                jnp.where(
                    first,
                    jnp.broadcast_to(delay[2 * i : 2 * i + 1], (8, LANES)),
                    jnp.broadcast_to(delay[2 * i + 1 : 2 * i + 2], (8, LANES)),
                )
                for i in range(n_all // 2)
            ],
            axis=0,
        )
        for c in range(cz):
            local = (lax.broadcasted_iota(jnp.int32, (1, LANES), 1) + c * LANES).astype(F32)
            fine = jnp.floor((local + 0.5) / COARSE)
            channel = (local - COARSE * fine) * (nz * fz) + fine + (chan * fz).astype(F32)
            frequency = (channel + 0.5) / (COARSE * nz * fz)
            cycles = delay * frequency
            turn = cycles - jnp.floor(cycles + 0.5)
            square = turn * turn
            w_re[c] = horner(COS_COEF, square)
            w_im[c] = turn * horner(SIN_COEF, square)

        def weigh(c, start, gain):
            rows = pl.ds(start, share)
            swapped = jnp.where(even, pltpu.roll(gain, share - 1, 0), -pltpu.roll(gain, 1, 0))
            weight = gain * w_re[c, rows, :] + swapped * w_im[c, rows, :]
            w_re[c, rows, :] = jnp.where(even, weight, pltpu.roll(weight, 1, 0))
            w_im[c, rows, :] = jnp.where(even, pltpu.roll(weight, share - 1, 0), weight)

        unroll = math.gcd(block, 8)

        def accumulate(slot, c, starts, extend, piece=None):
            def step(s, carry):
                sums = [[jnp.zeros((16, LANES), F32)] * 2 for _ in range(unroll)]
                for start in starts:
                    for q in range(share // 16):
                        at = start + q * 16
                        wr = w_re[c, pl.ds(at, 16), :]
                        wi = w_im[c, pl.ds(at, 16), :]
                        for u in range(unroll):
                            begin = pl.multiple_of((s * unroll + u) * rows_t + at, 16)
                            v = volt[slot, c, pl.ds(begin, 16), :].astype(F32)
                            sums[u] = [sums[u][0] + wr * v, sums[u][1] + wi * v]
                for u in range(unroll):
                    begin = pl.multiple_of((s * unroll + u) * 16, 16)
                    for which in range(2):
                        value = sums[u][which]
                        value = value[:8] + value[8:]
                        rows = pl.ds(begin + which * 8, 8)
                        acc[slot, c, rows, :] = acc[slot, c, rows, :] + value if extend else value
                return carry

            if piece is None:
                lax.fori_loop(0, block // unroll, step, 0)
            else:
                step(piece, 0)

        def take(slot, c, piece, which, p, ri):
            total = None
            for half in range(2):
                at = piece * unroll * 16 + which * 8 + half * 4 + p * 2 + ri
                value = acc[slot, c, pl.ds(at, unroll, stride=16), :]
                total = value if total is None else total + value
            return total

        starts = [0]
        if exchange:
            starts = [pl.multiple_of(lax.rem(beam + db, nb) * share, 16) for db in range(nb)]
        with jax.named_scope("acc1"):
            for c in range(cz):
                weigh(c, starts[0], gains[beam, c] if exchange else own_gain[c])
                if exchange:
                    wait_all(volt.at[:, c], volt_sem.at[c])

                    def first_sum(slot, carry, c=c):
                        accumulate(slot, c, starts[:1], False)
                        return carry

                    lax.fori_loop(0, chips, first_sum, 0)
        if pair > 1:

            @pl.when(jnp.logical_and(packs, chan < nz - 1))
            def _():
                with jax.named_scope("barrier2"):
                    pl.semaphore_wait(barrier, nt * nz - 1 + nb - 1)

            @pl.when(jnp.logical_and(packs, chan == nz - 1))
            def _():
                pl.semaphore_wait(ready, 1)

        for c in range(cz):
            with jax.named_scope(f"gainwait{c}"):
                if exchange:
                    wait_all(gains.at[pl.ds(0, nb - 1), c], gain_recv.at[c])
                else:
                    wait_all(volt.at[:, c], volt_sem.at[c])
            for db in range(1, nb if exchange else 1):
                weigh(c, starts[db], gains[lax.rem(beam + db, nb), c])
            for slot in range(chips):
                for piece in range(block // unroll):
                    rows = pl.ds(piece * unroll, unroll)
                    if exchange:
                        accumulate(slot, c, starts[1:], True, piece)
                    else:
                        accumulate(slot, c, starts, False, piece)
                    for p in range(2):
                        get = functools.partial(take, slot, c, piece)
                        part[slot, c, p * 2, rows] = get(0, p, 0) - get(1, p, 1)
                        part[slot, c, p * 2 + 1, rows] = get(0, p, 1) + get(1, p, 0)

                    def send(slot=slot, c=c, rows=rows):
                        pltpu.make_async_remote_copy(
                            src_ref=part.at[slot, c, :, rows],
                            dst_ref=recv.at[slot * pair + core, c, :, rows],
                            send_sem=send_sem.at[0],
                            recv_sem=part_recv.at[c],
                            device_id=peer(packer_of(chip_of(slot)), chan, beam),
                            device_id_type=MESH,
                        ).start()

                    if slot < chips - 1:
                        send()
                    elif pair > 1:
                        pl.when(jnp.logical_not(packs))(send)

        half = 2 * chan // nz
        place = chan * half + (nz - 1 - chan) * (1 - half)

        def target(i):
            if i == nz - 1:
                return chan
            other = i + (i + nz - place) // nz
            return other * half + (nz - 1 - other) * (1 - half)

        for copy in small[3:]:
            copy.wait()

        @pl.when(packs)
        def _():
            moved = jnp.zeros((4 * block, cz * LANES), F32)
            for c in range(cz):
                with jax.named_scope(f"partwait{c}"):
                    wait_all(recv.at[:, c], part_recv.at[c])
                sums = part[chips - 1, c]
                for i in range(nt - 1):
                    sums = sums + recv[i, c]
                sums = sums.reshape(4 * block, LANES)
                high = sums.astype(BF16)
                low = (sums - high.astype(F32)).astype(BF16)
                table = perm_ref[pl.ds(c * LANES, LANES), :]
                both = jnp.dot(
                    jnp.concatenate([high, low], axis=0), table, preferred_element_type=F32
                )
                moved = moved + both[: 4 * block] + both[4 * block :]
            group = lax.broadcasted_iota(jnp.int32, (block, LANES), 1) // fz
            quarter = 2 * lax.rem(chan, 2)
            turned = [
                [
                    pltpu.roll(
                        moved[g * block : (g + 1) * block, c * LANES : (c + 1) * LANES],
                        lax.rem(quarter + g, 4) * fz,
                        1,
                    )
                    for g in range(4)
                ]
                for c in range(cz)
            ]
            for i in range(nz):
                z = target(i)
                for c in range(cz):
                    total = turned[c][0]
                    for g in range(1, 4):
                        total = jnp.where(group == lax.rem(quarter + g + z, 4), turned[c][g], total)
                    packed[z, c] = total
                for back in range(reach + 1):
                    for k in range(pair) if back == 0 else range(pair - 1, -1, -1):
                        begin, size, start = rows_of(back, k)
                        if not size or (i == nz - 1 and back == 0 and k == packer):
                            continue

                        def send(i=i, back=back, k=k, begin=begin, size=size, start=start):
                            pltpu.make_async_remote_copy(
                                src_ref=packed.at[target(i), :, pl.ds(begin, size), :],
                                dst_ref=inbox.at[chan, :, pl.ds(start, size), :],
                                send_sem=send_sem.at[0],
                                recv_sem=pack_recv.at[back],
                                device_id=peer(lax.rem(chip + back, chips) * pair + k, target(i), beam),
                                device_id_type=MESH,
                            ).start()

                        if back == 0:
                            send()
                        else:
                            pl.when(chip + back < chips)(send)

            begin, size, start = rows_of(0, packer)
            inbox[chan, :, pl.ds(start, size), :] = packed[chan, :, pl.ds(begin, size), :]

        for copy in dft_copies:
            copy.wait()

    dma = pltpu.SemaphoreType.DMA
    pl.run_scoped(early, dma((5,)), dma((1,)), dma((cz,)), dma((1,)))

    def sent_rows(packing, reached):
        rows = (nb - 1) * cz * share if exchange else 0
        rows += (chips - packing) * cz * 4 * block
        if packing:
            for back in range(reached + 1):
                for k in range(pair):
                    count = nz - 1 if back == 0 and k == packer else nz
                    rows += count * cz * rows_of(back, k)[1]
        return rows

    def wait_sent(packing, reached):
        flat = acc.reshape(chips * cz * block * 16, LANES)
        wait_all(flat.at[pl.ds(0, sent_rows(packing, reached)), :], send_sem.at[0])

    with jax.named_scope("packwait"):
        for back in range(reach + 1):
            for k in range(pair):
                size, start = rows_of(back, k)[1:]
                if not size:
                    continue
                count = nz - 1 if back == 0 and k == packer else nz

                @pl.when(jnp.logical_and(core == k, chip >= back))
                def _(back=back, count=count, size=size, start=start):
                    wait_all(inbox.at[pl.ds(0, count), :, pl.ds(start, size), :], pack_recv.at[back])

    lane = lax.broadcasted_iota(jnp.int32, (span, LANES), 1) // fz
    early_half = lax.rem(lane + 4 - lax.rem(chan, 4), 4) < 2
    for p in range(2):
        lhs = jnp.concatenate(
            [
                jnp.concatenate(
                    [
                        jnp.where(early_half, inbox[2 * j + p, c], inbox[2 * j + 1 - p, c])
                        for j in range(nz // 2)
                    ],
                    axis=1,
                )
                for c in range(cz)
            ],
            axis=0,
        )
        high = lhs.astype(BF16)
        low = (lhs - high.astype(F32)).astype(BF16)
        dft_h, dft_l = [
            dft_ref[pl.ds(at + p * (nz // 2), nz // 2)].reshape(nz // 2 * 4 * fz, 2 * nz * fz)
            for at in (0, nz)
        ]
        both = jnp.dot(jnp.concatenate([high, low], axis=0), dft_h, preferred_element_type=F32)
        value = (
            both[: cz * span]
            + both[cz * span :]
            + jnp.dot(high, dft_l, preferred_element_type=F32)
        )
        for ri in range(2):
            spec[p * 2 + ri] = value[:, ri * LANES : (ri + 1) * LANES]
    for c in range(cz):
        for g in range(4):
            total = None
            for k in range(taps):
                value = synth_ref[pl.ds(k, 1), :] * spec[
                    g, pl.ds(c * span + halo * tb - k, tb), :
                ]
                total = value if total is None else total + value
            for t in range(tb):
                out_ref[t, c, pl.ds(g // 2, 1), (g % 2) * LANES : (g % 2 + 1) * LANES] = total[t : t + 1]

    with jax.named_scope("sendwait"):
        if pair > 1:
            pl.when(jnp.logical_not(packs))(functools.partial(wait_sent, 0, 0))
        for reached in range(min(reach, chips - 1) + 1):
            above = chips - 1 - chip
            here = above >= reach if reached == reach else above == reached
            pl.when(jnp.logical_and(packs, here))(functools.partial(wait_sent, 1, reached))


def store(value_ref, out_ref, sem):
    copy = pltpu.make_async_copy(value_ref, out_ref, sem)
    copy.start()
    copy.wait()


def body(mesh, voltages, calib_gain, tile_flags, delays, pointing, synth_filter):
    nt, nz, nb = mesh.shape["tile"], mesh.shape["chan"], mesh.shape["beam"]
    total_rows, n_all = voltages.shape[:2]
    width = voltages.shape[-1]
    taps, k = synth_filter.shape
    tb = total_rows // nt
    fz = width // COARSE
    cz = COARSE // nz
    halo = -(-(taps - 1) // tb)
    n_own = calib_gain.shape[0]
    exchange = n_own % 4 == 0 and mesh.shape["beam"] > 1
    gain = calib_gain
    if not exchange:
        gain = gain * tile_flags.astype(F32)[:, None, None, None]
        gain = lax.all_gather(gain, "beam", axis=0, tiled=True)
    perm = gather_table(nz, fz, cz)
    dft = np.concatenate(dft_table(nz, fz))
    cfg = (nt, nz, nb, tb, n_all, taps, fz, cz, halo, exchange)
    vmem = pl.BlockSpec(memory_space=pltpu.VMEM)
    anywhere = pl.BlockSpec(memory_space=pltpu.HBM)
    span = (halo + 1) * tb
    dma = pltpu.SemaphoreType.DMA
    pair = 2 if nt % 2 == 0 else 1
    chips = nt // pair
    reach = -(-(taps - 1) // (pair * tb))
    out = pl.pallas_call(
        functools.partial(kernel, cfg),
        out_shape=pltpu.VMEM((tb, cz, 2, 2 * k), F32),
        in_specs=[anywhere] * 8,
        out_specs=vmem,
        scratch_shapes=[
            pltpu.SMEM(tile_flags.shape, jnp.int32),
            pltpu.VMEM(delays.shape[::-1], F32),
            pltpu.SMEM(pointing.shape, jnp.int32),
            pltpu.VMEM(synth_filter.shape, F32),
            pltpu.VMEM(perm.shape, BF16),
            pltpu.VMEM(dft.shape, BF16),
            pltpu.VMEM((chips, cz, pair * tb * n_all * 4, LANES), BF16),
            pltpu.VMEM((cz, gain.shape[0] * 4, LANES), F32),
            pltpu.VMEM((nb, cz, n_own * 4, LANES), F32),
            pltpu.VMEM((cz, n_all * 4, LANES), F32),
            pltpu.VMEM((cz, n_all * 4, LANES), F32),
            pltpu.VMEM((chips, cz, pair * tb * 16, LANES), F32),
            pltpu.VMEM((chips, cz, 4, pair * tb, LANES), F32),
            pltpu.VMEM((nt - 1, cz, 4, pair * tb, LANES), F32),
            pltpu.VMEM((nz, cz, pair * tb, LANES), F32),
            pltpu.VMEM((nz, cz, span, LANES), F32),
            pltpu.VMEM((4, cz * span, k), F32),
            dma((1,)),
            dma((cz,)),
            dma((cz,)),
            dma((reach + 1,)),
            pltpu.SemaphoreType.REGULAR,
        ],
        compiler_params=pltpu.CompilerParams(collective_id=0, has_side_effects=True),
    )(
        voltages.reshape(-1, 2, width),
        gain.reshape(-1, 2, width),
        tile_flags,
        delays.T,
        pointing,
        synth_filter,
        jnp.asarray(perm),
        jnp.asarray(dft),
    )
    final = pl.pallas_call(
        store,
        out_shape=jax.ShapeDtypeStruct(out.shape, F32),
        in_specs=[vmem],
        out_specs=pl.BlockSpec(memory_space=pltpu.HBM),
        scratch_shapes=[dma(())],
    )(pltpu.with_memory_space_constraint(out, pltpu.VMEM))
    return final.transpose(0, 2, 1, 3)[:, None]


def solution(mesh):
    in_specs = (
        P(None, "tile", None, None, "chan"),
        P(("tile", "beam"), None, None, "chan"),
        P(("tile", "beam")),
        P(None, "tile"),
        P("beam"),
        P(),
    )
    out_specs = P("tile", "beam", None, "chan", None)
    return jax.shard_map(
        functools.partial(body, mesh), mesh=mesh, in_specs=in_specs, out_specs=out_specs, check_vma=False
    )
```

```python
import functools
import math

import jax
import jax.numpy as jnp
import numpy as np
from jax import lax
from jax.experimental import pallas as pl
from jax.experimental.pallas import tpu as pltpu
from jax.sharding import PartitionSpec as P

COARSE = 12
LANES = 128
MESH = pl.DeviceIdType.MESH
F32 = jnp.float32
BF16 = jnp.bfloat16


def even_fit(func, degree):
    series = np.polynomial.chebyshev.Chebyshev.interpolate(
        lambda u: func(np.sqrt(u)), degree, domain=[0.0, 0.25]
    )
    return [float(v) for v in series.convert(kind=np.polynomial.Polynomial).coef]


COS_COEF = even_fit(lambda r: np.cos(2 * np.pi * r), 7)
SIN_COEF = even_fit(lambda r: 2 * np.pi * np.sinc(2 * r), 7)


def horner(coef, u):
    total = jnp.full_like(u, coef[-1])
    for value in coef[-2::-1]:
        total = total * u + value
    return total


def split_bf16(table):
    high = table.astype(BF16)
    low = (table - high.astype(np.float64)).astype(BF16)
    return high, low


def dft_table(nz, fz):
    k = nz * fz
    f = np.arange(k)
    m = np.arange(k)
    angle = 2 * np.pi * (f[:, None] * m[None, :] % k) / k
    cosine, sine = np.cos(angle) / math.sqrt(k), np.sin(angle) / math.sqrt(k)
    cosine, sine = cosine.reshape(nz // 2, 2, fz, k), sine.reshape(nz // 2, 2, fz, k)
    out = np.zeros((2, nz // 2, 2, 2, fz, 2, k))
    for p in range(2):
        for odd in range(2):
            place = odd ^ p
            out[p, :, place, 0, :, 0], out[p, :, place, 0, :, 1] = cosine[:, odd], sine[:, odd]
            out[p, :, place, 1, :, 0], out[p, :, place, 1, :, 1] = -sine[:, odd], cosine[:, odd]
    return split_bf16(out.reshape(nz, 4, fz, 2 * k))


def gather_table(nz, fz, cz):
    width = fz * COARSE
    out = np.zeros((width, width), np.float64)
    for c in range(cz):
        for z in range(nz):
            for f in range(fz):
                out[f * COARSE + z * cz + c, (c * nz + z) * fz + f] = 1.0
    return out.astype(BF16)


def kernel(
    cfg,
    volt_ref,
    gain_ref,
    flag_src,
    delay_src,
    point_src,
    synth_src,
    perm_src,
    dft_src,
    out_ref,
    flag_ref,
    delay_ref,
    point_ref,
    synth_ref,
    perm_ref,
    dft_ref,
    volt,
    own_gain,
    gains,
    w_re,
    w_im,
    acc,
    part,
    recv,
    packed,
    inbox,
    spec,
    send_sem,
    gain_recv,
    part_recv,
    pack_recv,
    ready,
):
    nt, nz, nb, tb, n_all, taps, fz, cz, halo, exchange = cfg
    tile = lax.axis_index("tile")
    chan = lax.axis_index("chan")
    beam = lax.axis_index("beam")
    rows_t = n_all * 4

    def peer(t, z, b):
        return {"tile": t, "chan": z, "beam": b}

    pair = 2 if nt % 2 == 0 else 1
    chips = nt // pair
    chip, core = lax.div(tile, pair), lax.rem(tile, pair)
    packer = pair - 1
    packs = core == packer
    order = sorted(range(1, chips), key=lambda a: abs(2 * a - chips)) + [0]
    block = pair * tb

    def chip_of(slot):
        return lax.rem(chip + order[slot], chips)

    def packer_of(target_chip):
        return target_chip * pair + packer

    span = (halo + 1) * tb

    def wait_all(ref, sem):
        pltpu.make_async_copy(ref, ref, sem).wait()

    reach = -(-(taps - 1) // block)
    n_own = n_all // nb
    share = n_own * 4 if exchange else rows_t

    def rows_of(back, k):
        shift = (halo - k) * tb - back * block
        low = max(0, halo * tb - (taps - 1) - shift)
        high = min(block, (halo + 1) * tb - shift)
        return low, max(high - low, 0), low + shift

    def early(small_sem, own_sem, volt_sem, dft_sem):
        gain_rows = gain_ref.reshape(gain_ref.shape[0] * 2, gain_ref.shape[2])
        for c in range(cz):
            pltpu.make_async_copy(
                gain_rows.at[:, pl.ds(c * LANES, LANES)], own_gain.at[c], own_sem.at[0]
            ).start()
        small = [
            pltpu.make_async_copy(src, dst, small_sem.at[i])
            for i, (src, dst) in enumerate(
                [
                    (flag_src, flag_ref),
                    (point_src, point_ref),
                    (delay_src, delay_ref),
                    (synth_src, synth_ref),
                    (perm_src, perm_ref),
                ]
            )
        ]
        dft_copies = [
            pltpu.make_async_copy(
                dft_src.at[:, g], dft_ref.at[:, lax.rem(chan + g, 4)], dft_sem.at[0]
            )
            for g in range(4)
        ]
        for copy in small[:3]:
            copy.start()

        barrier = pltpu.get_barrier_semaphore()

        def greet(t, z, b):
            pl.semaphore_signal(barrier, inc=1, device_id=peer(t, z, b), device_id_type=MESH)

        for db in range(1, nb):
            greet(chip * pair, chan, lax.rem(beam + db, nb))
            if pair > 1:
                pl.when(packs)(functools.partial(greet, tile, chan, lax.rem(beam + db, nb)))
        if pair > 1:

            @pl.when(packs)
            def _():
                for a in range(chips):
                    for k in range(packer):
                        greet(lax.rem(chip + a, chips) * pair + k, chan, beam)

            @pl.when(jnp.logical_not(packs))
            def _():
                for a in range(chips):
                    greet(packer_of(lax.rem(chip + a, chips)), chan, beam)

        for dz in range(nz):
            for a in range(chips):
                if dz == 0:
                    if a:
                        pl.when(packs)(
                            functools.partial(greet, packer_of(lax.rem(chip + a, chips)), chan, beam)
                        )
                else:
                    greet(packer_of(lax.rem(chip + a, chips)), lax.rem(chan + dz, nz), beam)

        volt_rows = volt_ref.reshape(volt_ref.shape[0] * 2, volt_ref.shape[2])
        for c in range(cz):
            for slot in range(chips):
                pltpu.make_async_copy(
                    volt_rows.at[
                        pl.ds(chip_of(slot) * (block * rows_t), block * rows_t), pl.ds(c * LANES, LANES)
                    ],
                    volt.at[slot, c],
                    volt_sem.at[c],
                ).start()
        for copy in small[3:] + dft_copies:
            copy.start()

        row = lax.broadcasted_iota(jnp.int32, (8, LANES), 0)
        first = row < 4
        even = lax.rem(lax.broadcasted_iota(jnp.int32, (share, LANES), 0), 2) == 0

        with jax.named_scope("ownload"):
            wait_all(own_gain, own_sem.at[0])
            small[0].wait()
        if exchange:
            use = jnp.concatenate(
                [
                    jnp.where(first, flag_ref[2 * i].astype(F32), flag_ref[2 * i + 1].astype(F32))
                    for i in range(n_own // 2)
                ],
                axis=0,
            )
            for c in range(cz):
                gains[beam, c] = use * own_gain[c]

        with jax.named_scope("barrier"):
            if pair > 1:

                @pl.when(jnp.logical_not(packs))
                def _():
                    pl.semaphore_wait(barrier, chips + (nb - 1) * pair)
                    pl.semaphore_signal(
                        ready,
                        inc=1,
                        device_id=peer(packer_of(chip), chan, beam),
                        device_id_type=MESH,
                    )

                @pl.when(jnp.logical_and(packs, chan < nz - 1))
                def _():
                    pl.semaphore_wait(ready, 1)

                @pl.when(jnp.logical_and(packs, chan == nz - 1))
                def _():
                    pl.semaphore_wait(barrier, nt * nz - 1 + nb - 1)

            else:
                pl.semaphore_wait(barrier, nt * nz - 1 + nb - 1)

        if exchange:
            for c in range(cz):
                for db in range(1, nb):
                    pltpu.make_async_remote_copy(
                        src_ref=gains.at[beam, c],
                        dst_ref=gains.at[beam, c],
                        send_sem=send_sem.at[0],
                        recv_sem=gain_recv.at[c],
                        device_id=peer(tile, chan, lax.rem(beam + db, nb)),
                        device_id_type=MESH,
                    ).start()

        unused = halo * tb - (taps - 1)
        if unused:
            inbox[:, :, pl.ds(0, unused), :] = jnp.zeros((nz, cz, unused, LANES), F32)
        for back in range(1, reach + 1):
            for k in range(pair):
                size, start = rows_of(back, k)[1:]
                if size:

                    @pl.when(jnp.logical_and(chip < back, core == k))
                    def _(size=size, start=start):
                        inbox[:, :, pl.ds(start, size), :] = jnp.zeros((nz, cz, size, LANES), F32)

        for copy in small[1:3]:
            copy.wait()
        select = lax.broadcasted_iota(jnp.int32, delay_ref.shape, 1) == point_ref[0]
        delay = jnp.sum(jnp.where(select, delay_ref[...], 0.0), axis=1, keepdims=True)
        delay = jnp.broadcast_to(delay, (n_all, LANES))
        delay = jnp.concatenate(
            [
                jnp.where(
                    first,
                    jnp.broadcast_to(delay[2 * i : 2 * i + 1], (8, LANES)),
                    jnp.broadcast_to(delay[2 * i + 1 : 2 * i + 2], (8, LANES)),
                )
                for i in range(n_all // 2)
            ],
            axis=0,
        )
        for c in range(cz):
            local = (lax.broadcasted_iota(jnp.int32, (1, LANES), 1) + c * LANES).astype(F32)
            fine = jnp.floor((local + 0.5) / COARSE)
            channel = (local - COARSE * fine) * (nz * fz) + fine + (chan * fz).astype(F32)
            frequency = (channel + 0.5) / (COARSE * nz * fz)
            cycles = delay * frequency
            turn = cycles - jnp.floor(cycles + 0.5)
            square = turn * turn
            w_re[c] = horner(COS_COEF, square)
            w_im[c] = turn * horner(SIN_COEF, square)

        def weigh(c, start, gain):
            rows = pl.ds(start, share)
            swapped = jnp.where(even, pltpu.roll(gain, share - 1, 0), -pltpu.roll(gain, 1, 0))
            weight = gain * w_re[c, rows, :] + swapped * w_im[c, rows, :]
            w_re[c, rows, :] = jnp.where(even, weight, pltpu.roll(weight, 1, 0))
            w_im[c, rows, :] = jnp.where(even, pltpu.roll(weight, share - 1, 0), weight)

        unroll = math.gcd(block, 8)

        def accumulate(slot, c, starts, extend, piece=None):
            def step(s, carry):
                sums = [[jnp.zeros((16, LANES), F32)] * 2 for _ in range(unroll)]
                for start in starts:
                    for q in range(share // 16):
                        at = start + q * 16
                        wr = w_re[c, pl.ds(at, 16), :]
                        wi = w_im[c, pl.ds(at, 16), :]
                        for u in range(unroll):
                            begin = pl.multiple_of((s * unroll + u) * rows_t + at, 16)
                            v = volt[slot, c, pl.ds(begin, 16), :].astype(F32)
                            sums[u] = [sums[u][0] + wr * v, sums[u][1] + wi * v]
                for u in range(unroll):
                    begin = pl.multiple_of((s * unroll + u) * 16, 16)
                    for which in range(2):
                        value = sums[u][which]
                        value = value[:8] + value[8:]
                        rows = pl.ds(begin + which * 8, 8)
                        acc[slot, c, rows, :] = acc[slot, c, rows, :] + value if extend else value
                return carry

            if piece is None:
                lax.fori_loop(0, block // unroll, step, 0)
            else:
                step(piece, 0)

        def take(slot, c, piece, which, p, ri):
            total = None
            for half in range(2):
                at = piece * unroll * 16 + which * 8 + half * 4 + p * 2 + ri
                value = acc[slot, c, pl.ds(at, unroll, stride=16), :]
                total = value if total is None else total + value
            return total

        starts = [0]
        if exchange:
            starts = [pl.multiple_of(lax.rem(beam + db, nb) * share, 16) for db in range(nb)]
        with jax.named_scope("acc1"):
            for c in range(cz):
                weigh(c, starts[0], gains[beam, c] if exchange else own_gain[c])
                if exchange:
                    wait_all(volt.at[:, c], volt_sem.at[c])

                    def first_sum(slot, carry, c=c):
                        accumulate(slot, c, starts[:1], False)
                        return carry

                    lax.fori_loop(0, chips, first_sum, 0)
        if pair > 1:

            @pl.when(jnp.logical_and(packs, chan < nz - 1))
            def _():
                with jax.named_scope("barrier2"):
                    pl.semaphore_wait(barrier, nt * nz - 1 + nb - 1)

            @pl.when(jnp.logical_and(packs, chan == nz - 1))
            def _():
                pl.semaphore_wait(ready, 1)

        for c in range(cz):
            with jax.named_scope(f"gainwait{c}"):
                if exchange:
                    wait_all(gains.at[pl.ds(0, nb - 1), c], gain_recv.at[c])
                else:
                    wait_all(volt.at[:, c], volt_sem.at[c])
            for db in range(1, nb if exchange else 1):
                weigh(c, starts[db], gains[lax.rem(beam + db, nb), c])
            for slot in range(chips):
                for piece in range(block // unroll):
                    rows = pl.ds(piece * unroll, unroll)
                    if exchange:
                        accumulate(slot, c, starts[1:], True, piece)
                    else:
                        accumulate(slot, c, starts, False, piece)
                    for p in range(2):
                        get = functools.partial(take, slot, c, piece)
                        part[slot, c, p * 2, rows] = get(0, p, 0) - get(1, p, 1)
                        part[slot, c, p * 2 + 1, rows] = get(0, p, 1) + get(1, p, 0)

                    def send(slot=slot, c=c, rows=rows):
                        pltpu.make_async_remote_copy(
                            src_ref=part.at[slot, c, :, rows],
                            dst_ref=recv.at[slot * pair + core, c, :, rows],
                            send_sem=send_sem.at[0],
                            recv_sem=part_recv.at[c],
                            device_id=peer(packer_of(chip_of(slot)), chan, beam),
                            device_id_type=MESH,
                        ).start()

                    if slot < chips - 1:
                        send()
                    elif pair > 1:
                        pl.when(jnp.logical_not(packs))(send)

        half = 2 * chan // nz
        place = chan * half + (nz - 1 - chan) * (1 - half)

        def target(i):
            if i == nz - 1:
                return chan
            other = i + (i + nz - place) // nz
            return other * half + (nz - 1 - other) * (1 - half)

        for copy in small[3:]:
            copy.wait()

        @pl.when(packs)
        def _():
            moved = jnp.zeros((4 * block, cz * LANES), F32)
            for c in range(cz):
                with jax.named_scope(f"partwait{c}"):
                    wait_all(recv.at[:, c], part_recv.at[c])
                sums = part[chips - 1, c]
                for i in range(nt - 1):
                    sums = sums + recv[i, c]
                sums = sums.reshape(4 * block, LANES)
                high = sums.astype(BF16)
                low = (sums - high.astype(F32)).astype(BF16)
                table = perm_ref[pl.ds(c * LANES, LANES), :]
                both = jnp.dot(
                    jnp.concatenate([high, low], axis=0), table, preferred_element_type=F32
                )
                moved = moved + both[: 4 * block] + both[4 * block :]
            group = lax.broadcasted_iota(jnp.int32, (block, LANES), 1) // fz
            quarter = 2 * lax.rem(chan, 2)
            turned = [
                [
                    pltpu.roll(
                        moved[g * block : (g + 1) * block, c * LANES : (c + 1) * LANES],
                        lax.rem(quarter + g, 4) * fz,
                        1,
                    )
                    for g in range(4)
                ]
                for c in range(cz)
            ]
            for i in range(nz):
                z = target(i)
                for c in range(cz):
                    total = turned[c][0]
                    for g in range(1, 4):
                        total = jnp.where(group == lax.rem(quarter + g + z, 4), turned[c][g], total)
                    packed[z, c] = total
                for back in range(reach + 1):
                    for k in range(pair) if back == 0 else range(pair - 1, -1, -1):
                        begin, size, start = rows_of(back, k)
                        if not size or (i == nz - 1 and back == 0 and k == packer):
                            continue

                        def send(i=i, back=back, k=k, begin=begin, size=size, start=start):
                            pltpu.make_async_remote_copy(
                                src_ref=packed.at[target(i), :, pl.ds(begin, size), :],
                                dst_ref=inbox.at[chan, :, pl.ds(start, size), :],
                                send_sem=send_sem.at[0],
                                recv_sem=pack_recv.at[back],
                                device_id=peer(lax.rem(chip + back, chips) * pair + k, target(i), beam),
                                device_id_type=MESH,
                            ).start()

                        if back == 0:
                            send()
                        else:
                            pl.when(chip + back < chips)(send)

            begin, size, start = rows_of(0, packer)
            inbox[chan, :, pl.ds(start, size), :] = packed[chan, :, pl.ds(begin, size), :]

        for copy in dft_copies:
            copy.wait()

    dma = pltpu.SemaphoreType.DMA
    pl.run_scoped(early, dma((5,)), dma((1,)), dma((cz,)), dma((1,)))

    def sent_rows(packing, reached):
        rows = (nb - 1) * cz * share if exchange else 0
        rows += (chips - packing) * cz * 4 * block
        if packing:
            for back in range(reached + 1):
                for k in range(pair):
                    count = nz - 1 if back == 0 and k == packer else nz
                    rows += count * cz * rows_of(back, k)[1]
        return rows

    def wait_sent(packing, reached):
        flat = acc.reshape(chips * cz * block * 16, LANES)
        wait_all(flat.at[pl.ds(0, sent_rows(packing, reached)), :], send_sem.at[0])

    with jax.named_scope("packwait"):
        for back in range(reach + 1):
            for k in range(pair):
                size, start = rows_of(back, k)[1:]
                if not size:
                    continue
                count = nz - 1 if back == 0 and k == packer else nz

                @pl.when(jnp.logical_and(core == k, chip >= back))
                def _(back=back, count=count, size=size, start=start):
                    wait_all(inbox.at[pl.ds(0, count), :, pl.ds(start, size), :], pack_recv.at[back])

    lane = lax.broadcasted_iota(jnp.int32, (span, LANES), 1) // fz
    early_half = lax.rem(lane + 4 - lax.rem(chan, 4), 4) < 2
    for p in range(2):
        lhs = jnp.concatenate(
            [
                jnp.concatenate(
                    [
                        jnp.where(early_half, inbox[2 * j + p, c], inbox[2 * j + 1 - p, c])
                        for j in range(nz // 2)
                    ],
                    axis=1,
                )
                for c in range(cz)
            ],
            axis=0,
        )
        high = lhs.astype(BF16)
        low = (lhs - high.astype(F32)).astype(BF16)
        dft_h, dft_l = [
            dft_ref[pl.ds(at + p * (nz // 2), nz // 2)].reshape(nz // 2 * 4 * fz, 2 * nz * fz)
            for at in (0, nz)
        ]
        both = jnp.dot(jnp.concatenate([high, low], axis=0), dft_h, preferred_element_type=F32)
        value = (
            both[: cz * span]
            + both[cz * span :]
            + jnp.dot(high, dft_l, preferred_element_type=F32)
        )
        for ri in range(2):
            spec[p * 2 + ri] = value[:, ri * LANES : (ri + 1) * LANES]
    for c in range(cz):
        for g in range(4):
            total = None
            for k in range(taps):
                value = synth_ref[pl.ds(k, 1), :] * spec[
                    g, pl.ds(c * span + halo * tb - k, tb), :
                ]
                total = value if total is None else total + value
            for t in range(tb):
                out_ref[t, c, pl.ds(g // 2, 1), (g % 2) * LANES : (g % 2 + 1) * LANES] = total[t : t + 1]

    with jax.named_scope("sendwait"):
        if pair > 1:
            pl.when(jnp.logical_not(packs))(functools.partial(wait_sent, 0, 0))
        for reached in range(min(reach, chips - 1) + 1):
            above = chips - 1 - chip
            here = above >= reach if reached == reach else above == reached
            pl.when(jnp.logical_and(packs, here))(functools.partial(wait_sent, 1, reached))


def store(value_ref, out_ref, sem):
    copy = pltpu.make_async_copy(value_ref, out_ref, sem)
    copy.start()
    copy.wait()


def body(mesh, voltages, calib_gain, tile_flags, delays, pointing, synth_filter):
    nt, nz, nb = mesh.shape["tile"], mesh.shape["chan"], mesh.shape["beam"]
    total_rows, n_all = voltages.shape[:2]
    width = voltages.shape[-1]
    taps, k = synth_filter.shape
    tb = total_rows // nt
    fz = width // COARSE
    cz = COARSE // nz
    halo = -(-(taps - 1) // tb)
    n_own = calib_gain.shape[0]
    exchange = n_own % 4 == 0 and mesh.shape["beam"] > 1
    gain = calib_gain
    if not exchange:
        gain = gain * tile_flags.astype(F32)[:, None, None, None]
        gain = lax.all_gather(gain, "beam", axis=0, tiled=True)
    perm = gather_table(nz, fz, cz)
    dft = np.concatenate(dft_table(nz, fz))
    cfg = (nt, nz, nb, tb, n_all, taps, fz, cz, halo, exchange)
    vmem = pl.BlockSpec(memory_space=pltpu.VMEM)
    anywhere = pl.BlockSpec(memory_space=pltpu.HBM)
    span = (halo + 1) * tb
    dma = pltpu.SemaphoreType.DMA
    pair = 2 if nt % 2 == 0 else 1
    chips = nt // pair
    reach = -(-(taps - 1) // (pair * tb))
    out = pl.pallas_call(
        functools.partial(kernel, cfg),
        out_shape=pltpu.VMEM((tb, cz, 2, 2 * k), F32),
        in_specs=[anywhere] * 8,
        out_specs=vmem,
        scratch_shapes=[
            pltpu.SMEM(tile_flags.shape, jnp.int32),
            pltpu.VMEM(delays.shape[::-1], F32),
            pltpu.SMEM(pointing.shape, jnp.int32),
            pltpu.VMEM(synth_filter.shape, F32),
            pltpu.VMEM(perm.shape, BF16),
            pltpu.VMEM(dft.shape, BF16),
            pltpu.VMEM((chips, cz, pair * tb * n_all * 4, LANES), BF16),
            pltpu.VMEM((cz, gain.shape[0] * 4, LANES), F32),
            pltpu.VMEM((nb, cz, n_own * 4, LANES), F32),
            pltpu.VMEM((cz, n_all * 4, LANES), F32),
            pltpu.VMEM((cz, n_all * 4, LANES), F32),
            pltpu.VMEM((chips, cz, pair * tb * 16, LANES), F32),
            pltpu.VMEM((chips, cz, 4, pair * tb, LANES), F32),
            pltpu.VMEM((nt - 1, cz, 4, pair * tb, LANES), F32),
            pltpu.VMEM((nz, cz, pair * tb, LANES), F32),
            pltpu.VMEM((nz, cz, span, LANES), F32),
            pltpu.VMEM((4, cz * span, k), F32),
            dma((1,)),
            dma((cz,)),
            dma((cz,)),
            dma((reach + 1,)),
            pltpu.SemaphoreType.REGULAR,
        ],
        compiler_params=pltpu.CompilerParams(collective_id=0, has_side_effects=True),
    )(
        voltages.reshape(-1, 2, width),
        gain.reshape(-1, 2, width),
        tile_flags,
        delays.T,
        pointing,
        synth_filter,
        jnp.asarray(perm),
        jnp.asarray(dft),
    )
    final = pl.pallas_call(
        store,
        out_shape=jax.ShapeDtypeStruct(out.shape, F32),
        in_specs=[vmem],
        out_specs=pl.BlockSpec(memory_space=pltpu.HBM),
        scratch_shapes=[dma(())],
    )(pltpu.with_memory_space_constraint(out, pltpu.VMEM))
    return final.transpose(0, 2, 1, 3)[:, None]


def solution(mesh):
    in_specs = (
        P(None, "tile", None, None, "chan"),
        P(("tile", "beam"), None, None, "chan"),
        P(("tile", "beam")),
        P(None, "tile"),
        P("beam"),
        P(),
    )
    out_specs = P("tile", "beam", None, "chan", None)
    return jax.shard_map(
        functools.partial(body, mesh), mesh=mesh, in_specs=in_specs, out_specs=out_specs, check_vma=False
    )
```
